64 devices in a mesh: data: 4 (over x, y), ctx: 16 (over z, core).
Axes of the slice: x: 2, y: 2, z: 8, core: 2. Of those that a mesh axis runs over, the one named last changes fastest.
The devices are a block of a 4x4x8 slice.
Arguments:
- queries: bfloat16 [4, 32768, 2, 256], P('data', 'ctx'), parts along dimension 0
- key_rows: bfloat16 [4, 32768, 1, 256], P('data', 'ctx'), parts along dimension 0
- value_rows: bfloat16 [4, 32768, 1, 256], P('data', 'ctx'), parts along dimension 0
Outputs:
- output: bfloat16 [4, 32768, 2, 256], P('data', 'ctx'), parts along dimension 0
There are 4 independent parts. The reference program is written for one: setup_inputs(seed, part) draws one part's arguments, and reference() takes and returns one part's arrays. A program takes and returns all parts, laid end to end along the dimension named above; each array names one.
All inputs are finite; a program needn't handle non-finite values.
Results may differ from the reference program's by a relative error of at most 0.00204687.
Values are sent between devices in bfloat16 or wider.
A program may use at most 768 MiB of HBM per device.

```python
import math
import jax
import jax.numpy as jnp
from jax import lax

BATCH = 1
CHUNK = 2048
GROUP = 16
HEADS = 2
KV_HEADS = 1
HEAD = 256

SEQ = GROUP * CHUNK
RATIO = HEADS // KV_HEADS
KEY_TILE = min(CHUNK, 256)
N_TILES = SEQ // KEY_TILE
SCORE_SCALE = 1.0 / math.sqrt(HEAD)


def setup_inputs(seed: int = 0, part: int = 0) -> dict:
    base_key = jax.random.fold_in(jax.random.key(seed), part)
    key_q, key_k, key_v, key_off = jax.random.split(base_key, 4)
    queries = jax.random.normal(key_q, (BATCH, SEQ, HEADS, HEAD), jnp.float32)
    key_rows = jax.random.normal(key_k, (BATCH, SEQ, KV_HEADS, HEAD), jnp.float32)
    value_noise = jax.random.normal(key_v, (BATCH, GROUP, CHUNK, KV_HEADS, HEAD), jnp.float32)
    piece_offset = jax.random.normal(key_off, (BATCH, GROUP, 1, KV_HEADS, HEAD), jnp.float32)
    value_rows = (0.5 * value_noise + piece_offset).reshape(BATCH, SEQ, KV_HEADS, HEAD)
    return {
        "queries": queries.astype(jnp.bfloat16),
        "key_rows": key_rows.astype(jnp.bfloat16),
        "value_rows": value_rows.astype(jnp.bfloat16),
    }


def reference(queries, key_rows, value_rows):
    q_pieces = queries.reshape(BATCH, GROUP, CHUNK, KV_HEADS, RATIO, HEAD)
    k_tiles = key_rows.reshape(BATCH, N_TILES, KEY_TILE, KV_HEADS, HEAD)
    v_tiles = value_rows.reshape(BATCH, N_TILES, KEY_TILE, KV_HEADS, HEAD)
    local_pos = jnp.arange(CHUNK)
    tile_pos = jnp.arange(KEY_TILE)

    def query_piece(q_idx):
        q_blk = lax.dynamic_index_in_dim(q_pieces, q_idx, axis=1, keepdims=False).astype(jnp.float32)
        q_pos = q_idx * CHUNK + local_pos
        init_state = (
            jnp.zeros((BATCH, CHUNK, KV_HEADS, RATIO, HEAD), jnp.float32),
            jnp.full((BATCH, KV_HEADS, RATIO, CHUNK), -jnp.inf, jnp.float32),
            jnp.zeros((BATCH, KV_HEADS, RATIO, CHUNK), jnp.float32),
        )

        def update(state_now, t_idx):
            o_acc, m_acc, l_acc = state_now
            k_tile = lax.dynamic_index_in_dim(k_tiles, t_idx, axis=1, keepdims=False).astype(jnp.float32)
            v_tile = lax.dynamic_index_in_dim(v_tiles, t_idx, axis=1, keepdims=False).astype(jnp.float32)
            k_pos = t_idx * KEY_TILE + tile_pos
            scores = jnp.einsum("bqhgd,bkhd->bhgqk", q_blk, k_tile) * SCORE_SCALE
            scores = jnp.where(q_pos[:, None] >= k_pos[None, :], scores, -jnp.inf)
            m_new = jnp.maximum(m_acc, jnp.max(scores, axis=-1))
            rescale = jnp.exp(m_acc - m_new)
            exp_scores = jnp.exp(scores - m_new[..., None])
            l_new = l_acc * rescale + jnp.sum(exp_scores, axis=-1)
            pv_part = jnp.einsum("bhgqk,bkhd->bqhgd", exp_scores, v_tile)
            o_new = o_acc * jnp.transpose(rescale, (0, 3, 1, 2))[..., None] + pv_part
            return (o_new, m_new, l_new)

        def keep_state(state_now, t_idx):
            return state_now

        def key_step(state_in, t_idx):
            needed = t_idx * KEY_TILE <= q_idx * CHUNK + CHUNK - 1
            new_state = lax.cond(needed, update, keep_state, state_in, t_idx)
            return new_state, None

        final_state, unused_out = lax.scan(key_step, init_state, jnp.arange(N_TILES))
        o_acc, m_acc, l_acc = final_state
        return (o_acc / jnp.transpose(l_acc, (0, 3, 1, 2))[..., None]).astype(jnp.bfloat16)

    pieces = lax.map(query_piece, jnp.arange(GROUP))
    return jnp.moveaxis(pieces, 0, 1).reshape(BATCH, SEQ, HEADS, HEAD)
```

```python
import functools
import math

import jax
import jax.numpy as jnp
from jax import lax
from jax.experimental import pallas as pl
from jax.experimental.pallas import tpu as pltpu
from jax.sharding import PartitionSpec as P

MESH = pl.DeviceIdType.MESH
CP = 8
NT = (((1,), (1,)), ((), ()))
NN = (((1,), (0,)), ((), ()))


def kernel(n, scale2, q_hbm, k_hbm, v_hbm, out_hbm,
           kv, qraw, q_s, oraw, acc, m_s, l_s, s_s, mx_s, vt_s,
           load_sem, qload_sem, recv_sem, qrecv_sem, orecv_sem, ostore_sem,
           up_sem, dn_sem, sib_sem, qsend_sem, osend_sem):
    me = lax.axis_index("ctx")
    chip, core = me // 2, me % 2
    sib = 1 - core
    half = n // 2
    n_pos = CP * (n - 1) // 2
    own0 = n_pos
    ch = k_hbm.shape[1]
    d = k_hbm.shape[2]
    rows = q_s.shape[1]
    gk = 4 * ch

    def dev(c, k):
        return {"ctx": c * 2 + k}

    sib_dev = dev(chip, sib)
    above = lax.rem(chip + 1, n)
    below = lax.rem(chip + n - 1, n)
    up_dev, dn_dev = dev(above, core), dev(below, core)
    low = chip < half

    def up_count(c):
        return jnp.where(c < half, c * CP, c * (CP // 2))

    def up_slot(c, u):
        lo = c < half
        return jnp.where(lo, u // 2, u), jnp.where(lo, 2 * (u % 2) + core, core)

    n_up = up_count(chip)
    n_up_above = jnp.where(chip + 1 < n, up_count(chip + 1), 0)
    n_dn = jnp.where(low, 0, chip * (CP // 2))
    n_dn_below = jnp.where(chip - 1 < half, 0, (chip - 1) * (CP // 2))
    n_steps = chip * (CP // 2)
    transit0 = CP * (chip + 1)
    n_transit = jnp.where(low, jnp.maximum(n_pos - transit0, 0), 0)

    def own_chunk(j):
        jj = core * CP + j
        return own0 + jj // 4, jj % 4

    def sib_chunk(j):
        jj = sib * CP + j
        return own0 + jj // 4, jj % 4

    def block_row(j):
        return 2 * j + lax.rem(core + j, 2)

    def send(slot_from, slot_to, sem, device):
        return pltpu.make_async_remote_copy(
            src_ref=kv.at[slot_from[0], slot_from[1]], dst_ref=kv.at[slot_to[0], slot_to[1]],
            send_sem=sem, recv_sem=recv_sem.at[slot_to[0], slot_to[1]],
            device_id=device, device_id_type=MESH)

    def arrived(slot):
        send(slot, slot, sib_sem, sib_dev).wait_recv()

    loads = []
    for j in range(CP):
        a, b = own_chunk(j)
        loads.append((pltpu.make_async_copy(k_hbm.at[j], kv.at[a, b, 0], load_sem.at[j, 0]),
                      pltpu.make_async_copy(v_hbm.at[j], kv.at[a, b, 1], load_sem.at[j, 1])))
    for j in reversed(range(CP)):
        loads[j][0].start()
        loads[j][1].start()
    qloads = []
    for i in range(CP // 2):
        j = core * (CP // 2) + i
        qloads.append(pltpu.make_async_copy(q_hbm.at[block_row(j) - core * CP], qraw.at[j], qload_sem.at[i]))
        qloads[-1].start()

    barrier = pltpu.get_barrier_semaphore()
    for device in (sib_dev, up_dev, dn_dev):
        pl.semaphore_signal(barrier, inc=1, device_id=device, device_id_type=MESH)
    pl.semaphore_wait(barrier, 3)

    def q_give(i):
        j = core * (CP // 2) + i
        row = 2 * j + lax.rem(sib + j, 2) - core * CP
        return pltpu.make_async_remote_copy(
            src_ref=q_hbm.at[row], dst_ref=qraw.at[j], send_sem=qsend_sem.at[i], recv_sem=qrecv_sem.at[i],
            device_id=sib_dev, device_id_type=MESH)

    def q_take(i):
        j = sib * (CP // 2) + i
        return pltpu.make_async_remote_copy(
            src_ref=q_hbm.at[0], dst_ref=qraw.at[j], send_sem=qsend_sem.at[i], recv_sem=qrecv_sem.at[i],
            device_id=sib_dev, device_id_type=MESH)

    for u in range(CP):
        j = CP - 1 - u
        loads[j][0].wait()
        loads[j][1].wait()

        @pl.when(u < n_up_above)
        def _():
            send(own_chunk(j), up_slot(chip + 1, u), up_sem, up_dev).start()

    first_dn = chip * CP
    for j in range(CP):
        @pl.when(first_dn + j < n_pos)
        def _():
            send(own_chunk(j), (first_dn + j, 2 + core), dn_sem, dn_dev).start()
    for i in range(CP // 2):
        q_give(i).start()
    for j in range(CP):
        send(own_chunk(j), own_chunk(j), sib_sem, sib_dev).start()

    def serve_up(p):
        @pl.when(p < n_up)
        def _():
            slot = up_slot(chip, p)
            arrived(slot)

            @pl.when(p + CP < n_up_above)
            def _():
                send(slot, up_slot(chip + 1, p + CP), up_sem, up_dev).start()
            send(slot, slot, sib_sem, sib_dev).start()

    def serve_dn(p):
        @pl.when(p < n_dn)
        def _():
            slot = (p, 2 + core)
            arrived(slot)

            @pl.when(p < n_dn_below)
            def _():
                send(slot, slot, dn_sem, dn_dev).start()
            send(slot, slot, sib_sem, sib_dev).start()

    def serve_transit(p):
        @pl.when(p < n_transit)
        def _():
            slot = (transit0 + p, 2 + core)
            arrived(slot)
            send(slot, slot, dn_sem, dn_dev).start()

    def serve(s):
        @pl.when(low)
        def _():
            for i in range(2):
                serve_transit(2 * s + i)
            for i in range(2):
                serve_up(2 * s + i)

        @pl.when(jnp.logical_not(low))
        def _():
            serve_up(s)
            serve_dn(s)

    def wait_sibling(s):
        @pl.when(s < n_steps)
        def _():
            arrived((s, sib))
            arrived((s, 2 + sib))

    def qk(j, g, c0, nk, slot, off):
        k = kv[g, c0:c0 + nk // ch, 0].reshape(nk, d)
        s = lax.dot_general(k, q_s[j], NT, preferred_element_type=jnp.float32)
        if off is not None:
            key = lax.broadcasted_iota(jnp.int32, (nk, rows), 0)
            tok = lax.broadcasted_iota(jnp.int32, (nk, rows), 1) // 2
            s = jnp.where(key - tok <= off, s, -jnp.inf)
        s_s[slot, 0:nk] = s
        mx_s[slot] = jnp.max(s.reshape(nk // 8, 8, rows), axis=0)

    def sm_pv(j, v, c0, nk, slot):
        m_old = m_s[j]
        m_new = jnp.maximum(m_old, jnp.max(mx_s[slot], axis=0, keepdims=True))
        alpha = jnp.exp2((m_old - m_new) * scale2)
        m_s[j] = m_new
        p = jnp.exp2((s_s[slot, 0:nk].reshape(nk // 8, 8, rows) - m_new[None]) * scale2)
        l_s[j] = l_s[j] * alpha + jnp.sum(p, axis=0)
        pv = lax.dot_general(vt_s[v, :, c0 * ch:c0 * ch + nk], p.reshape(nk, rows).astype(jnp.bfloat16), NN,
                             preferred_element_type=jnp.float32)
        acc[j] = (acc[j].reshape(d // 8, 8, rows) * alpha[None]).reshape(d, rows) + pv

    def make_vt(g, v):
        vt_s[v] = kv[g, :, 1].reshape(gk, d).T

    def run(tiles, nxt=None):
        for t, (j, g, c0, nk, off, v) in enumerate(tiles):
            if t + 1 < len(tiles):
                j1, g1, c1, nk1, off1, _ = tiles[t + 1]
                qk(j1, g1, c1, nk1, (t + 1) % 2, off1)
            elif nxt is not None:
                qk(0, nxt, 0, gk, (t + 1) % 2, None)
            sm_pv(j, v, c0, nk, t % 2)

    m_s[...] = jnp.full_like(m_s, -jnp.inf)
    l_s[...] = jnp.zeros_like(l_s)
    acc[...] = jnp.zeros_like(acc)

    def triangle(h):
        for i in range(CP // 2):
            j = h * (CP // 2) + i
            q_s[j] = qraw[j].reshape(rows, d)
        tiles = []
        off_even = ch * core
        off_odd = ch * (3 - core)
        for e in range(2):
            make_vt(own0 + 2 * h + e, e)
        for i in range(CP // 2):
            j = h * (CP // 2) + i
            for e in range(i // 2):
                tiles.append((j, own0 + 2 * h + e, 0, gk, None, e))
            e = i // 2
            if i % 2 == 0:
                tiles.append((j, own0 + 2 * h + e, 0, 2 * ch, off_even, e))
            else:
                tiles.append((j, own0 + 2 * h + e, 0, gk, off_odd, e))
        qk(tiles[0][0], tiles[0][1], tiles[0][2], tiles[0][3], 0, tiles[0][4])
        run(tiles)

    def both_triangles(r, carry):
        h = lax.rem(core + r, 2)

        @pl.when(r == 0)
        def _():
            for cp in qloads:
                cp.wait()

        @pl.when(r == 1)
        def _():
            for i in range(CP // 2):
                q_take(i).wait_recv()
            for j in range(CP):
                arrived(sib_chunk(j))
        triangle(h)
        return carry

    lax.fori_loop(0, 2, both_triangles, 0)
    serve(0)

    def next_group(s):
        return jnp.where(s < n_steps, s, own0)

    for e in range(2):
        make_vt(own0 + e, e)
    tiles = [(j, own0 + e, 0, gk, None, e) for e in range(2) for j in range(CP // 2, CP)]
    qk(tiles[0][0], tiles[0][1], 0, gk, 0, None)
    run(tiles[:-1], None)
    wait_sibling(0)
    g0 = next_group(0)
    qk(tiles[-1][0], tiles[-1][1], 0, gk, 1, None)
    qk(0, g0, 0, gk, 0, None)
    sm_pv(tiles[-1][0], 1, 0, gk, 1)
    make_vt(g0, 0)

    def step(s, carry):
        v = lax.rem(s, 2)
        t = lambda j: (j, s, 0, gk, None, v)
        for j in range(4):
            qk(j + 1, s, 0, gk, (j + 1) % 2, None)
            sm_pv(j, v, 0, gk, j % 2)
        serve(s + 1)
        for j in range(4, CP - 1):
            qk(j + 1, s, 0, gk, (j + 1) % 2, None)
            sm_pv(j, v, 0, gk, j % 2)
        wait_sibling(s + 1)
        g = next_group(s + 1)
        qk(0, g, 0, gk, 0, None)
        make_vt(g, 1 - v)
        sm_pv(CP - 1, v, 0, gk, 1)
        return carry

    lax.fori_loop(0, n_steps, step, 0)

    n_serve = jnp.maximum(n_steps, (n_transit + 1) // 2)

    def rest(s, carry):
        serve(s + 1)
        return carry

    lax.fori_loop(n_steps, n_serve, rest, 0)

    def o_home(i):
        j = core * (CP // 2) + i
        return pltpu.make_async_copy(oraw.at[j], out_hbm.at[block_row(j) - core * CP], ostore_sem.at[i])

    def o_give(i):
        j = sib * (CP // 2) + i
        return pltpu.make_async_remote_copy(
            src_ref=oraw.at[j], dst_ref=out_hbm.at[block_row(j) - sib * CP], send_sem=osend_sem.at[i],
            recv_sem=orecv_sem.at[i], device_id=sib_dev, device_id_type=MESH)

    def o_take(i):
        j = core * (CP // 2) + i
        row = 2 * j + lax.rem(sib + j, 2) - core * CP
        return pltpu.make_async_remote_copy(
            src_ref=oraw.at[j], dst_ref=out_hbm.at[row], send_sem=osend_sem.at[i],
            recv_sem=orecv_sem.at[i], device_id=sib_dev, device_id_type=MESH)

    def finish(j):
        inv = 1.0 / jnp.sum(l_s[j], axis=0, keepdims=True)
        o = acc[j] * inv
        oraw[j] = o.T.astype(jnp.bfloat16).reshape(ch, rows // ch, d)

    for i in range(CP // 2):
        finish(sib * (CP // 2) + i)
        o_give(i).start()
    for i in range(CP // 2):
        finish(core * (CP // 2) + i)
        o_home(i).start()

    def drain(count, sem):
        def one(i, carry):
            send((own0, 0), (own0, 0), sem, sib_dev).wait_send()
            return carry
        lax.fori_loop(0, count, one, 0)

    own_up = jnp.minimum(n_up_above, CP)
    own_dn = jnp.clip(n_pos - first_dn, 0, CP)
    drain(own_up + jnp.clip(n_up_above - CP, 0, n_up), up_sem)
    drain(own_dn + n_dn_below + n_transit, dn_sem)
    drain(CP + n_up + n_dn, sib_sem)
    for i in range(CP // 2):
        q_give(i).wait_send()
        o_give(i).wait_send()
        o_home(i).wait()
        o_take(i).wait_recv()


def solution(mesh):
    n = mesh.shape["ctx"] // 2
    seq_spec = P("data", "ctx", None, None)

    def local_attention(queries, key_rows, value_rows):
        n_batch, chunk_len, n_heads, head_dim = queries.shape
        ch = chunk_len // CP
        rows = ch * n_heads
        n_pos = CP * (n - 1) // 2
        bf16, f32 = jnp.bfloat16, jnp.float32
        hbm = pl.BlockSpec(memory_space=pltpu.HBM)
        dma = pltpu.SemaphoreType.DMA
        out = pl.pallas_call(
            functools.partial(kernel, n, math.log2(math.e) / math.sqrt(head_dim)),
            out_shape=jax.ShapeDtypeStruct((CP, ch, n_heads, head_dim), bf16),
            in_specs=[hbm, hbm, hbm],
            out_specs=hbm,
            scratch_shapes=[
                pltpu.VMEM((n_pos + 4, 4, 2, ch, head_dim), bf16),
                pltpu.VMEM((CP, ch, n_heads, head_dim), bf16),
                pltpu.VMEM((CP, rows, head_dim), bf16),
                pltpu.VMEM((CP, ch, n_heads, head_dim), bf16),
                pltpu.VMEM((CP, head_dim, rows), f32),
                pltpu.VMEM((CP, 8, rows), f32),
                pltpu.VMEM((CP, 8, rows), f32),
                pltpu.VMEM((2, 4 * ch, rows), f32),
                pltpu.VMEM((2, 8, rows), f32),
                pltpu.VMEM((2, head_dim, 4 * ch), bf16),
                dma((CP, 2)), dma((CP // 2,)), dma((n_pos + 4, 4)), dma((CP // 2,)), dma((CP // 2,)), dma((CP // 2,)),
                dma, dma, dma, dma((CP // 2,)), dma((CP // 2,)),
            ],
            compiler_params=pltpu.CompilerParams(
                collective_id=0, has_side_effects=True, vmem_limit_bytes=60 * 1024 * 1024),
            name="attention",
        )(queries.reshape(CP, ch, n_heads, head_dim), key_rows.reshape(CP, ch, head_dim),
          value_rows.reshape(CP, ch, head_dim))
        return out.reshape(queries.shape)

    return jax.shard_map(local_attention, mesh=mesh, in_specs=(seq_spec, seq_spec, seq_spec),
                         out_specs=seq_spec, check_vma=False)
```

```python
import functools
import math

import jax
import jax.numpy as jnp
from jax import lax
from jax.experimental import pallas as pl
from jax.experimental.pallas import tpu as pltpu
from jax.sharding import PartitionSpec as P

MESH = pl.DeviceIdType.MESH
CP = 8
NT = (((1,), (1,)), ((), ()))
NN = (((1,), (0,)), ((), ()))


def kernel(n, scale2, q_hbm, k_hbm, v_hbm, out,
           kv, qraw, q_s, ostage, acc, m_s, l_s, s_s, mx_s, vt_s,
           load_sem, qload_sem, recv_sem, qrecv_sem, orecv_sem,
           fwd_sem, sib_sem, qsend_sem, osend_sem):
    me = lax.axis_index("ctx")
    chip, core = me // 2, me % 2
    sib = 1 - core
    half = n // 2
    n_pos = CP * (n - 1) // 2
    own0 = n_pos
    ch = k_hbm.shape[1]
    d = k_hbm.shape[2]
    rows = q_s.shape[1]
    gk = 4 * ch

    def dev(c, k):
        return {"ctx": c * 2 + k}

    sib_dev = dev(chip, sib)
    above = lax.rem(chip + 1, n)
    below = lax.rem(chip + n - 1, n)
    up_dev, dn_dev = dev(above, core), dev(below, core)
    low = chip < half

    def up_count(c):
        return jnp.where(c < half, c * CP, c * (CP // 2))

    def up_slot(c, u):
        lo = c < half
        return jnp.where(lo, u // 2, u), jnp.where(lo, 2 * (u % 2) + core, core)

    n_up = up_count(chip)
    n_up_above = jnp.where(chip + 1 < n, up_count(chip + 1), 0)
    n_dn = jnp.where(low, 0, chip * (CP // 2))
    n_dn_below = jnp.where(chip - 1 < half, 0, (chip - 1) * (CP // 2))
    n_steps = chip * (CP // 2)
    transit0 = CP * (chip + 1)
    n_transit = jnp.where(low, jnp.maximum(n_pos - transit0, 0), 0)

    def own_chunk(j):
        jj = core * CP + j
        return own0 + jj // 4, jj % 4

    def sib_chunk(j):
        jj = sib * CP + j
        return own0 + jj // 4, jj % 4

    def block_row(j):
        return 2 * j + lax.rem(core + j, 2)

    def send(slot_from, slot_to, sem, device):
        return pltpu.make_async_remote_copy(
            src_ref=kv.at[slot_from[0], slot_from[1]], dst_ref=kv.at[slot_to[0], slot_to[1]],
            send_sem=sem, recv_sem=recv_sem.at[slot_to[0], slot_to[1]],
            device_id=device, device_id_type=MESH)

    def arrived(slot):
        send(slot, slot, sib_sem, sib_dev).wait_recv()

    loads = []
    for j in range(CP):
        a, b = own_chunk(j)
        loads.append((pltpu.make_async_copy(k_hbm.at[j], kv.at[a, b, 0], load_sem.at[j, 0]),
                      pltpu.make_async_copy(v_hbm.at[j], kv.at[a, b, 1], load_sem.at[j, 1])))
    for j in reversed(range(CP)):
        loads[j][0].start()
        loads[j][1].start()
    qloads = []
    for i in range(CP // 2):
        j = core * (CP // 2) + i
        qloads.append(pltpu.make_async_copy(q_hbm.at[block_row(j) - core * CP], qraw.at[j], qload_sem.at[i]))
        qloads[-1].start()

    barrier = pltpu.get_barrier_semaphore()
    for device in (sib_dev, up_dev, dn_dev):
        pl.semaphore_signal(barrier, inc=1, device_id=device, device_id_type=MESH)
    pl.semaphore_wait(barrier, 3)

    def q_give(i):
        j = core * (CP // 2) + i
        row = 2 * j + lax.rem(sib + j, 2) - core * CP
        return pltpu.make_async_remote_copy(
            src_ref=q_hbm.at[row], dst_ref=qraw.at[j], send_sem=qsend_sem.at[i], recv_sem=qrecv_sem.at[i],
            device_id=sib_dev, device_id_type=MESH)

    def q_take(i):
        j = sib * (CP // 2) + i
        return pltpu.make_async_remote_copy(
            src_ref=q_hbm.at[0], dst_ref=qraw.at[j], send_sem=qsend_sem.at[i], recv_sem=qrecv_sem.at[i],
            device_id=sib_dev, device_id_type=MESH)

    for u in range(CP):
        j = CP - 1 - u
        loads[j][0].wait()
        loads[j][1].wait()

        @pl.when(u < n_up_above)
        def _():
            send(own_chunk(j), up_slot(chip + 1, u), fwd_sem, up_dev).start()

    first_dn = chip * CP
    for j in range(CP):
        @pl.when(first_dn + j < n_pos)
        def _():
            send(own_chunk(j), (first_dn + j, 2 + core), fwd_sem, dn_dev).start()
    for i in range(CP // 2):
        q_give(i).start()
    for j in range(CP):
        send(own_chunk(j), own_chunk(j), sib_sem, sib_dev).start()

    def serve(s):
        lo = low.astype(jnp.int32)
        p1 = s + lo * s
        p2 = p1 + lo
        slot1 = (s, core)
        slot2 = (s, 2 + core)
        have1 = p1 < n_up
        have2 = jnp.where(low, p2 < n_up, p2 < n_dn)
        fwd1 = jnp.logical_and(have1, p1 + CP < n_up_above)
        fwd2 = jnp.logical_and(have2, jnp.where(low, p2 + CP < n_up_above, p2 < n_dn_below))
        to1 = up_slot(chip + 1, p1 + CP)
        up2 = up_slot(chip + 1, p2 + CP)
        to2 = (jnp.where(low, up2[0], p2), jnp.where(low, up2[1], 2 + core))
        dev2 = dev(jnp.where(low, above, below), core)
        have3 = s < n_transit
        slot3 = (jnp.minimum(transit0 + s, n_pos - 1), 2 + core)

        @pl.when(have1)
        def _():
            arrived(slot1)

        @pl.when(fwd1)
        def _():
            send(slot1, to1, fwd_sem, up_dev).start()

        @pl.when(have1)
        def _():
            send(slot1, slot1, sib_sem, sib_dev).start()

        @pl.when(have2)
        def _():
            arrived(slot2)

        @pl.when(fwd2)
        def _():
            send(slot2, to2, fwd_sem, dev2).start()

        @pl.when(have2)
        def _():
            send(slot2, slot2, sib_sem, sib_dev).start()

        @pl.when(have3)
        def _():
            arrived(slot3)

        @pl.when(have3)
        def _():
            send(slot3, slot3, fwd_sem, dn_dev).start()

    def wait_sibling(s):
        arrived((s, sib))
        arrived((s, 2 + sib))

    def qk(j, g, c0, nk, slot, off):
        k = kv[g, c0:c0 + nk // ch, 0].reshape(nk, d)
        s = lax.dot_general(k, q_s[j], NT, preferred_element_type=jnp.float32)
        if off is not None:
            key = lax.broadcasted_iota(jnp.int32, (nk, rows), 0)
            tok = lax.broadcasted_iota(jnp.int32, (nk, rows), 1) // 2
            s = jnp.where(key - tok <= off, s, -jnp.inf)
        s_s[slot, 0:nk] = s
        mx_s[slot] = jnp.max(s.reshape(nk // 8, 8, rows), axis=0)

    def sm_pv(j, v, c0, nk, slot):
        m_old = m_s[j]
        m_new = jnp.maximum(m_old, jnp.max(mx_s[slot], axis=0, keepdims=True))
        alpha = jnp.exp2((m_old - m_new) * scale2)
        m_s[j] = m_new
        p = jnp.exp2((s_s[slot, 0:nk].reshape(nk // 8, 8, rows) - m_new[None]) * scale2)
        l_s[j] = l_s[j] * alpha + jnp.sum(p, axis=0)
        pv = lax.dot_general(vt_s[v, :, c0 * ch:c0 * ch + nk], p.reshape(nk, rows).astype(jnp.bfloat16), NN,
                             preferred_element_type=jnp.float32)
        acc[j] = (acc[j].reshape(d // 8, 8, rows) * alpha[None]).reshape(d, rows) + pv

    def make_vt(g, v):
        vt_s[v] = kv[g, :, 1].reshape(gk, d).T

    own_v = 2

    def run(tiles, last=True):
        qk(*tiles[0][:4], 0, tiles[0][4])
        for t, (j, g, c0, nk, off, v) in enumerate(tiles):
            if t + 1 < len(tiles):
                qk(*tiles[t + 1][:4], (t + 1) % 2, tiles[t + 1][4])
            elif not last:
                break
            sm_pv(j, v, c0, nk, t % 2)

    m_s[...] = jnp.full_like(m_s, -jnp.inf)
    l_s[...] = jnp.zeros_like(l_s)
    acc[...] = jnp.zeros_like(acc)

    def triangle(h):
        for i in range(CP // 2):
            j = h * (CP // 2) + i
            q_s[j] = qraw[j].reshape(rows, d)
        tiles = []
        off_even = ch * core
        off_odd = ch * (3 - core)
        for e in range(2):
            make_vt(own0 + 2 * h + e, own_v + 2 * h + e)
        for i in range(CP // 2):
            j = h * (CP // 2) + i
            for e in range(i // 2):
                tiles.append((j, own0 + 2 * h + e, 0, gk, None, own_v + 2 * h + e))
            e = i // 2
            if i % 2 == 0:
                tiles.append((j, own0 + 2 * h + e, 0, 2 * ch, off_even, own_v + 2 * h + e))
            else:
                tiles.append((j, own0 + 2 * h + e, 0, gk, off_odd, own_v + 2 * h + e))
        run(tiles)

    def both_triangles(r, carry):
        h = lax.rem(core + r, 2)

        @pl.when(r == 0)
        def _():
            for cp in qloads:
                cp.wait()

        @pl.when(r == 1)
        def _():
            for i in range(CP // 2):
                q_take(i).wait_recv()
            for j in range(CP):
                arrived(sib_chunk(j))
        triangle(h)
        return carry

    lax.fori_loop(0, 2, both_triangles, 0)
    serve(0)

    run([(j, own0 + e, 0, gk, None, own_v + e) for e in range(2) for j in range(CP // 2, CP)], last=False)

    def step_tiles(s, blocks, before_j, before_v, after):
        wait_sibling(s)
        v = lax.rem(s, 2)
        make_vt(s, v)
        qk(blocks[0], s, 0, gk, 0, None)
        sm_pv(before_j, before_v, 0, gk, 1)
        for i in range(CP - 1):
            if i == CP // 2:
                serve(s + 1)
            qk(blocks[i + 1], s, 0, gk, (i + 1) % 2, None)
            sm_pv(blocks[i], v, 0, gk, i % 2)
            after(i)

    def before(s):
        return jnp.where(s == 0, own_v + 1, 1 - lax.rem(s, 2))

    def step(s, carry):
        step_tiles(s, range(CP), CP - 1, before(s), lambda i: None)
        return carry

    lax.fori_loop(0, n_steps - 1, step, 0)

    order = [sib * (CP // 2) + i for i in range(CP // 2)] + [core * (CP // 2) + i for i in range(CP // 2)]

    def o_give(i):
        return pltpu.make_async_remote_copy(
            src_ref=ostage.at[i], dst_ref=out.at[block_row(order[i]) - sib * CP], send_sem=osend_sem.at[i],
            recv_sem=orecv_sem.at[i], device_id=sib_dev, device_id_type=MESH)

    def o_take(i):
        j = core * (CP // 2) + i
        row = 2 * j + lax.rem(sib + j, 2) - core * CP
        return pltpu.make_async_remote_copy(
            src_ref=ostage.at[i], dst_ref=out.at[row], send_sem=osend_sem.at[i],
            recv_sem=orecv_sem.at[i], device_id=sib_dev, device_id_type=MESH)

    def finish(i):
        j = order[i]
        inv = 1.0 / jnp.sum(l_s[j], axis=0, keepdims=True)
        o = (acc[j] * inv).T.astype(jnp.bfloat16).reshape(ch, rows // ch, d)
        if i < CP // 2:
            ostage[i] = o
        else:
            out[block_row(j) - core * CP] = o
        if 1 <= i <= CP // 2:
            o_give(i - 1).start()

    @pl.when(n_steps > 0)
    def _():
        s = n_steps - 1
        step_tiles(s, order, CP - 1, before(s), finish)
        sm_pv(order[CP - 1], lax.rem(s, 2), 0, gk, 1)
        finish(CP - 1)

    @pl.when(n_steps == 0)
    def _():
        sm_pv(CP - 1, own_v + 1, 0, gk, 1)
        for i in range(CP):
            finish(i)

    def rest(s, carry):
        serve(s + 1)
        return carry

    lax.fori_loop(n_steps, jnp.maximum(n_steps, n_transit), rest, 0)

    def drain(count, sem):
        def one(i, carry):
            send((own0, 0), (own0, 0), sem, sib_dev).wait_send()
            return carry
        lax.fori_loop(0, count, one, 0)

    own_up = jnp.minimum(n_up_above, CP)
    own_dn = jnp.clip(n_pos - first_dn, 0, CP)
    drain(own_up + jnp.clip(n_up_above - CP, 0, n_up) + own_dn + n_dn_below + n_transit, fwd_sem)
    drain(CP + n_up + n_dn, sib_sem)
    for i in range(CP // 2):
        q_give(i).wait_send()
        o_give(i).wait_send()
        o_take(i).wait_recv()


def store_kernel(o_ref, out_hbm, sem):
    copy = pltpu.make_async_copy(o_ref, out_hbm, sem)
    copy.start()
    copy.wait()


def solution(mesh):
    n = mesh.shape["ctx"] // 2
    seq_spec = P("data", "ctx", None, None)

    def local_attention(queries, key_rows, value_rows):
        n_batch, chunk_len, n_heads, head_dim = queries.shape
        ch = chunk_len // CP
        rows = ch * n_heads
        n_pos = CP * (n - 1) // 2
        bf16, f32 = jnp.bfloat16, jnp.float32
        hbm = pl.BlockSpec(memory_space=pltpu.HBM)
        dma = pltpu.SemaphoreType.DMA
        out = pl.pallas_call(
            functools.partial(kernel, n, math.log2(math.e) / math.sqrt(head_dim)),
            out_shape=pltpu.VMEM((CP, ch, n_heads, head_dim), bf16),
            in_specs=[hbm, hbm, hbm],
            out_specs=pl.BlockSpec(memory_space=pltpu.VMEM),
            scratch_shapes=[
                pltpu.VMEM((n_pos + 4, 4, 2, ch, head_dim), bf16),
                pltpu.VMEM((CP, ch, n_heads, head_dim), bf16),
                pltpu.VMEM((CP, rows, head_dim), bf16),
                pltpu.VMEM((CP // 2, ch, n_heads, head_dim), bf16),
                pltpu.VMEM((CP, head_dim, rows), f32),
                pltpu.VMEM((CP, 8, rows), f32),
                pltpu.VMEM((CP, 8, rows), f32),
                pltpu.VMEM((2, 4 * ch, rows), f32),
                pltpu.VMEM((2, 8, rows), f32),
                pltpu.VMEM((6, head_dim, 4 * ch), bf16),
                dma((CP, 2)), dma((CP // 2,)), dma((n_pos + 4, 4)), dma((CP // 2,)), dma((CP // 2,)),
                dma, dma, dma((CP // 2,)), dma((CP // 2,)),
            ],
            compiler_params=pltpu.CompilerParams(
                collective_id=0, has_side_effects=True, vmem_limit_bytes=54 * 1024 * 1024),
            name="attention",
        )(queries.reshape(CP, ch, n_heads, head_dim), key_rows.reshape(CP, ch, head_dim),
          value_rows.reshape(CP, ch, head_dim))
        out = pl.pallas_call(
            store_kernel,
            out_shape=jax.ShapeDtypeStruct((CP, ch, n_heads, head_dim), bf16),
            in_specs=[pl.BlockSpec(memory_space=pltpu.VMEM)],
            out_specs=hbm,
            scratch_shapes=[dma],
            name="store",
        )(pltpu.with_memory_space_constraint(out, pltpu.VMEM))
        return out.reshape(queries.shape)

    return jax.shard_map(local_attention, mesh=mesh, in_specs=(seq_spec, seq_spec, seq_spec),
                         out_specs=seq_spec, check_vma=False)
```

```python
import functools
import math

import jax
import jax.numpy as jnp
from jax import lax
from jax.experimental import pallas as pl
from jax.experimental.pallas import tpu as pltpu
from jax.sharding import PartitionSpec as P

MESH = pl.DeviceIdType.MESH
CP = 8
EXTRA = 2
NT = (((1,), (1,)), ((), ()))
NN = (((1,), (0,)), ((), ()))


def kernel(n, scale2, q_hbm, k_hbm, v_hbm, out,
           kv, qraw, q_s, acc, m_s, l_s, s_s, mx_s, vt_s,
           load_sem, qload_sem, recv_sem, qrecv_sem, orecv_sem,
           fwd_sem, sib_sem, qsend_sem, osend_sem):
    me = lax.axis_index("ctx")
    chip, core = me // 2, me % 2
    sib = 1 - core
    half = n // 2
    hb = CP // 2
    n_pos = CP * (n - 1) // 2
    own0 = n_pos
    ch = k_hbm.shape[1]
    d = k_hbm.shape[2]
    rows = q_s.shape[1]
    gk = 4 * ch

    def dev(c, k):
        return {"ctx": c * 2 + k}

    sib_dev = dev(chip, sib)
    above = lax.rem(chip + 1, n)
    below = lax.rem(chip + n - 1, n)
    up_dev, dn_dev = dev(above, core), dev(below, core)
    low = chip < half

    def extra(c):
        return jnp.where(c == n - 1, 1 - core, EXTRA)

    def up_count(c):
        return jnp.where(c < half, c * CP, c * hb + extra(c))

    def up_slot(c, u):
        lo = c < half
        over = jnp.logical_and(jnp.logical_not(lo), u >= c * hb)
        row = jnp.where(lo, u // 2, jnp.where(over, u - extra(c), u))
        return row, jnp.where(lo, 2 * (u % 2) + core, jnp.where(over, 2 + core, core))

    dn_top = n_pos - extra(n - 1)
    n_up = up_count(chip)
    n_up_above = jnp.where(chip + 1 < n, up_count(chip + 1), 0)
    n_dn_below = jnp.where(chip - 1 < half, 0, (chip - 1) * hb - extra(chip - 1))
    n_steps = chip * hb
    transit0 = CP * (chip + 1)
    n_transit = jnp.where(low, jnp.maximum(dn_top - transit0, 0), 0)

    def chunk_slot(k, j):
        jj = k * CP + j
        return own0 + jj // 4, jj % 4

    def block_row(k, i):
        return 2 * (i % hb) + lax.rem(k + i, 2)

    def send(slot_from, slot_to, sem, device):
        return pltpu.make_async_remote_copy(
            src_ref=kv.at[slot_from[0], slot_from[1]], dst_ref=kv.at[slot_to[0], slot_to[1]],
            send_sem=sem, recv_sem=recv_sem.at[slot_to[0], slot_to[1]],
            device_id=device, device_id_type=MESH)

    def arrived(slot):
        send(slot, slot, sib_sem, sib_dev).wait_recv()

    def share(slot):
        send(slot, slot, sib_sem, sib_dev).start()

    loads = []
    for j in range(CP):
        a, b = chunk_slot(core, j)
        loads.append((pltpu.make_async_copy(k_hbm.at[j], kv.at[a, b, 0], load_sem.at[j, 0]),
                      pltpu.make_async_copy(v_hbm.at[j], kv.at[a, b, 1], load_sem.at[j, 1])))
    for j in reversed(range(CP)):
        loads[j][0].start()
        loads[j][1].start()
    qloads = [pltpu.make_async_copy(q_hbm.at[block_row(core, hb + i)], qraw.at[hb + i], qload_sem.at[i])
              for i in range(hb)]
    for copy in qloads:
        copy.start()

    barrier = pltpu.get_barrier_semaphore()
    for device in (sib_dev, up_dev, dn_dev):
        pl.semaphore_signal(barrier, inc=1, device_id=device, device_id_type=MESH)
    pl.semaphore_wait(barrier, 3)

    def q_give(i):
        return pltpu.make_async_remote_copy(
            src_ref=q_hbm.at[block_row(sib, i)], dst_ref=qraw.at[i], send_sem=qsend_sem.at[i], recv_sem=qrecv_sem.at[i],
            device_id=sib_dev, device_id_type=MESH)

    first_dn = chip * CP
    for u in range(CP):
        j = CP - 1 - u
        loads[j][0].wait()
        loads[j][1].wait()

        @pl.when(u < n_up_above)
        def _():
            send(chunk_slot(core, j), up_slot(chip + 1, u), fwd_sem, up_dev).start()
    for j in range(CP):
        @pl.when(first_dn + j < dn_top)
        def _():
            send(chunk_slot(core, j), (first_dn + j, 2 + core), fwd_sem, dn_dev).start()
    for i in range(hb):
        q_give(i).start()
    for j in range(CP):
        share(chunk_slot(core, j))

    def take(s):
        arrived((s, core))
        share((s, core))
        arrived((s, 2 + core))
        share((s, 2 + core))

    def transit(s):
        @pl.when(s < n_transit)
        def _():
            slot = (jnp.minimum(transit0 + s, n_pos - 1), 2 + core)
            arrived(slot)
            send(slot, slot, fwd_sem, dn_dev).start()

    def forward(s):
        lo = low.astype(jnp.int32)
        p1 = s + lo * s
        p2 = p1 + lo
        up2 = up_slot(chip + 1, p2 + CP)
        to2 = (jnp.where(low, up2[0], s), jnp.where(low, up2[1], 2 + core))
        dev2 = dev(jnp.where(low, above, below), core)

        @pl.when(p1 + CP < n_up_above)
        def _():
            send((s, core), up_slot(chip + 1, p1 + CP), fwd_sem, up_dev).start()

        @pl.when(jnp.where(low, p2 + CP < n_up_above, s < n_dn_below))
        def _():
            send((s, 2 + core), to2, fwd_sem, dev2).start()
        transit(s)

    def qk(i, g, nk, slot, off):
        k = kv[g, 0:nk // ch, 0].reshape(nk, d)
        s = lax.dot_general(k, q_s[i], NT, preferred_element_type=jnp.float32)
        if off is not None:
            key = lax.broadcasted_iota(jnp.int32, (nk, rows), 0)
            tok = lax.broadcasted_iota(jnp.int32, (nk, rows), 1) // 2
            s = jnp.where(key - tok <= off, s, -jnp.inf)
        s_s[slot, 0:nk] = s
        mx_s[slot] = jnp.max(s.reshape(nk // 8, 8, rows), axis=0)

    def sm_pv(i, v, nk, slot, first=False):
        m_new = jnp.max(mx_s[slot], axis=0, keepdims=True)
        if first:
            m_new = jnp.broadcast_to(m_new, (8, rows))
        else:
            m_old = m_s[i]
            m_new = jnp.maximum(m_old, m_new)
            alpha = jnp.exp2((m_old - m_new) * scale2)
        m_s[i] = m_new
        p = jnp.exp2((s_s[slot, 0:nk].reshape(nk // 8, 8, rows) - m_new[None]) * scale2)
        l_new = jnp.sum(p, axis=0)
        pv = lax.dot_general(vt_s[v, :, 0:nk], p.reshape(nk, rows).astype(jnp.bfloat16), NN,
                             preferred_element_type=jnp.float32)
        if first:
            l_s[i] = l_new
            acc[i] = pv
        else:
            l_s[i] = l_s[i] * alpha + l_new
            acc[i] = (acc[i].reshape(d // 8, 8, rows) * alpha[None]).reshape(d, rows) + pv

    def make_vt(g, v):
        vt_s[v] = kv[g, :, 1].reshape(gk, d).T

    own_v = 2

    def run(tiles, last=True):
        qk(*tiles[0][:3], 0, tiles[0][3])
        for t, (i, g, nk, off, v, first) in enumerate(tiles):
            if t + 1 < len(tiles):
                qk(*tiles[t + 1][:3], (t + 1) % 2, tiles[t + 1][3])
            elif not last:
                break
            sm_pv(i, v, nk, t % 2, first)

    def triangle(k, i0):
        for i in range(hb):
            q_s[i0 + i] = qraw[i0 + i].reshape(rows, d)
        for e in range(2):
            make_vt(own0 + 2 * k + e, own_v + 2 * k + e)
        tiles = []
        for i in range(hb):
            for e in range(i // 2 + 1):
                g, v = own0 + 2 * k + e, own_v + 2 * k + e
                if e < i // 2:
                    tiles.append((i0 + i, g, gk, None, v, e == 0))
                elif i % 2 == 0:
                    tiles.append((i0 + i, g, 2 * ch, ch * core, v, e == 0))
                else:
                    tiles.append((i0 + i, g, gk, ch * (3 - core), v, e == 0))
        run(tiles)

    for copy in qloads:
        copy.wait()
    triangle(core, hb)
    for i in range(hb):
        q_give(i).wait_recv()
    for j in range(CP):
        arrived(chunk_slot(sib, j))
    triangle(sib, 0)

    @pl.when(n_steps > 0)
    def _():
        take(0)

    run([(hb * core + i, own0 + e, gk, None, own_v + e, False) for e in range(2) for i in range(hb)], last=False)

    def step_tiles(s, before, mid, after):
        arrived((s, sib))
        arrived((s, 2 + sib))
        forward(s)
        v = lax.rem(s, 2)
        make_vt(s, v)
        qk(0, s, gk, 0, None)
        sm_pv(*before, gk, 1)
        for i in range(CP - 1):
            if i == hb:
                mid()
            qk(i + 1, s, gk, (i + 1) % 2, None)
            sm_pv(i, v, gk, i % 2)
            after(i)

    def before(s):
        first = s == 0
        return (jnp.where(first, hb * core + hb - 1, CP - 1), jnp.where(first, own_v + 1, 1 - lax.rem(s, 2)))

    def step(s, carry):
        step_tiles(s, before(s), lambda: take(s + 1), lambda i: None)
        return carry

    lax.fori_loop(0, n_steps - 1, step, 0)

    def o_give(i):
        return pltpu.make_async_remote_copy(
            src_ref=out.at[CP + i], dst_ref=out.at[block_row(core, i)], send_sem=osend_sem.at[i],
            recv_sem=orecv_sem.at[i], device_id=sib_dev, device_id_type=MESH)

    def o_take(i):
        return pltpu.make_async_remote_copy(
            src_ref=out.at[CP + i], dst_ref=out.at[block_row(sib, i)], send_sem=osend_sem.at[i],
            recv_sem=orecv_sem.at[i], device_id=sib_dev, device_id_type=MESH)

    def finish(i):
        inv = 1.0 / jnp.sum(l_s[i], axis=0, keepdims=True)
        o = (acc[i] * inv).astype(jnp.bfloat16).T.reshape(ch, rows // ch, d)
        out[CP + i if i < hb else block_row(core, i)] = o

    def finish_send(i):
        finish(i)
        if i == hb:
            for k in range(hb):
                o_give(k).start()

    @pl.when(n_steps > 0)
    def _():
        s = n_steps - 1
        step_tiles(s, before(s), lambda: None, finish_send)
        sm_pv(CP - 1, lax.rem(s, 2), gk, 1)
        finish_send(CP - 1)

    @pl.when(n_steps == 0)
    def _():
        sm_pv(hb * core + hb - 1, own_v + 1, gk, 1)
        for i in range(CP):
            finish_send(i)

    def rest(s, carry):
        transit(s)
        return carry

    lax.fori_loop(n_steps, jnp.maximum(n_steps, n_transit), rest, 0)

    def drain(count, sem):
        def one(i, carry):
            send((own0, 0), (own0, 0), sem, sib_dev).wait_send()
            return carry
        lax.fori_loop(0, count, one, 0)

    own_up = jnp.minimum(n_up_above, CP)
    own_dn = jnp.clip(dn_top - first_dn, 0, CP)
    drain(own_up + jnp.clip(n_up_above - CP, 0, n_up) + own_dn + n_dn_below + n_transit, fwd_sem)
    drain(CP + 2 * n_steps, sib_sem)
    for i in range(hb):
        q_give(i).wait_send()
        o_give(i).wait_send()
        o_take(i).wait_recv()


def store_kernel(o_ref, out_hbm, sem):
    copy = pltpu.make_async_copy(o_ref.at[0:out_hbm.shape[0]], out_hbm, sem)
    copy.start()
    copy.wait()


def solution(mesh):
    n = mesh.shape["ctx"] // 2
    seq_spec = P("data", "ctx", None, None)

    def local_attention(queries, key_rows, value_rows):
        n_batch, chunk_len, n_heads, head_dim = queries.shape
        ch = chunk_len // CP
        rows = ch * n_heads
        n_pos = CP * (n - 1) // 2
        bf16, f32 = jnp.bfloat16, jnp.float32
        hbm = pl.BlockSpec(memory_space=pltpu.HBM)
        dma = pltpu.SemaphoreType.DMA
        out = pl.pallas_call(
            functools.partial(kernel, n, math.log2(math.e) / math.sqrt(head_dim)),
            out_shape=pltpu.VMEM((CP + CP // 2, ch, n_heads, head_dim), bf16),
            in_specs=[hbm, hbm, hbm],
            out_specs=pl.BlockSpec(memory_space=pltpu.VMEM),
            scratch_shapes=[
                pltpu.VMEM((n_pos + 4, 4, 2, ch, head_dim), bf16),
                pltpu.VMEM((CP, ch, n_heads, head_dim), bf16),
                pltpu.VMEM((CP, rows, head_dim), bf16),
                pltpu.VMEM((CP, head_dim, rows), f32),
                pltpu.VMEM((CP, 8, rows), f32),
                pltpu.VMEM((CP, 8, rows), f32),
                pltpu.VMEM((2, 4 * ch, rows), f32),
                pltpu.VMEM((2, 8, rows), f32),
                pltpu.VMEM((6, head_dim, 4 * ch), bf16),
                dma((CP, 2)), dma((CP // 2,)), dma((n_pos + 4, 4)), dma((CP // 2,)), dma((CP // 2,)),
                dma, dma, dma((CP // 2,)), dma((CP // 2,)),
            ],
            compiler_params=pltpu.CompilerParams(
                collective_id=0, has_side_effects=True, vmem_limit_bytes=54 * 1024 * 1024),
            name="attention",
        )(queries.reshape(CP, ch, n_heads, head_dim), key_rows.reshape(CP, ch, head_dim),
          value_rows.reshape(CP, ch, head_dim))
        out = pl.pallas_call(
            store_kernel,
            out_shape=jax.ShapeDtypeStruct((CP, ch, n_heads, head_dim), bf16),
            in_specs=[pl.BlockSpec(memory_space=pltpu.VMEM)],
            out_specs=hbm,
            scratch_shapes=[dma],
            name="store",
        )(pltpu.with_memory_space_constraint(out, pltpu.VMEM))
        return out.reshape(queries.shape)

    return jax.shard_map(local_attention, mesh=mesh, in_specs=(seq_spec, seq_spec, seq_spec),
                         out_specs=seq_spec, check_vma=False)
```

```python
import functools
import math

import jax
import jax.numpy as jnp
from jax import lax
from jax.experimental import pallas as pl
from jax.experimental.pallas import tpu as pltpu
from jax.sharding import PartitionSpec as P

MESH = pl.DeviceIdType.MESH
CP = 8
EXTRA = 2
NT = (((1,), (1,)), ((), ()))
NN = (((1,), (0,)), ((), ()))


def kernel(n, scale2, q_hbm, k_hbm, v_hbm, out,
           kv, qraw, q_s, acc, m_s, l_s, s_s, mx_s, vt_s,
           load_sem, qload_sem, recv_sem, qrecv_sem, orecv_sem,
           fwd_sem, sib_sem, qsend_sem, osend_sem):
    me = lax.axis_index("ctx")
    chip, core = me // 2, me % 2
    sib = 1 - core
    half = n // 2
    hb = CP // 2
    n_pos = CP * (n - 1) // 2
    own0 = n_pos + 1
    ch = k_hbm.shape[1]
    d = k_hbm.shape[2]
    rows = q_s.shape[1]
    gk = 4 * ch

    def dev(c, k):
        return {"ctx": c * 2 + k}

    sib_dev = dev(chip, sib)
    above = lax.rem(chip + 1, n)
    below = lax.rem(chip + n - 1, n)
    up_dev, dn_dev = dev(above, core), dev(below, core)
    low = chip < half

    def extra(c):
        return jnp.where(c == n - 1, 1 - core, EXTRA)

    def up_count(c):
        return jnp.where(c < half, c * CP, c * hb + extra(c))

    def up_slot(c, u):
        lo = c < half
        over = jnp.logical_and(jnp.logical_not(lo), u >= c * hb)
        row = jnp.where(lo, u // 2, jnp.where(over, u - extra(c), u))
        return row, jnp.where(lo, u % 2, over.astype(jnp.int32))

    dn_top = n_pos - extra(n - 1)
    n_up = up_count(chip)
    n_up_above = jnp.where(chip + 1 < n, up_count(chip + 1), 0)
    n_dn_below = jnp.where(chip - 1 < half, 0, (chip - 1) * hb - extra(chip - 1))
    n_steps = chip * hb
    transit0 = CP * (chip + 1)
    n_transit = jnp.where(low, jnp.maximum(dn_top - transit0, 0), 0)

    def chunk_slot(k, j):
        jj = k * CP + j
        return own0 + jj // 4, jj % 4

    def block_row(k, i):
        return 2 * (i % hb) + lax.rem(k + i, 2)

    def send(slot_from, slot_to, sem, device):
        return pltpu.make_async_remote_copy(
            src_ref=kv.at[slot_from[0], slot_from[1]], dst_ref=kv.at[slot_to[0], slot_to[1]],
            send_sem=sem, recv_sem=recv_sem.at[slot_to[0], slot_to[1]],
            device_id=device, device_id_type=MESH)

    def arrived(slot):
        send(slot, slot, sib_sem, sib_dev).wait_recv()

    def share(slot):
        send(slot, slot, sib_sem, sib_dev).start()

    loads = []
    for j in range(CP):
        a, b = chunk_slot(core, j)
        loads.append((pltpu.make_async_copy(k_hbm.at[j], kv.at[a, b, 0], load_sem.at[j, 0]),
                      pltpu.make_async_copy(v_hbm.at[j], kv.at[a, b, 1], load_sem.at[j, 1])))
    for j in reversed(range(CP)):
        loads[j][0].start()
        loads[j][1].start()
    qloads = [pltpu.make_async_copy(q_hbm.at[block_row(core, hb + i)], qraw.at[hb + i], qload_sem.at[i])
              for i in range(hb)]
    for copy in qloads:
        copy.start()

    barrier = pltpu.get_barrier_semaphore()
    for device in (sib_dev, up_dev, dn_dev):
        pl.semaphore_signal(barrier, inc=1, device_id=device, device_id_type=MESH)
    pl.semaphore_wait(barrier, 3)

    def q_give(i):
        return pltpu.make_async_remote_copy(
            src_ref=q_hbm.at[block_row(sib, i)], dst_ref=qraw.at[i], send_sem=qsend_sem.at[i], recv_sem=qrecv_sem.at[i],
            device_id=sib_dev, device_id_type=MESH)

    first_dn = chip * CP
    for u in range(CP):
        j = CP - 1 - u
        loads[j][0].wait()
        loads[j][1].wait()

        @pl.when(u < n_up_above)
        def _():
            send(chunk_slot(core, j), up_slot(chip + 1, u), fwd_sem, up_dev).start()
    for j in range(CP):
        @pl.when(first_dn + j < dn_top)
        def _():
            send(chunk_slot(core, j), (first_dn + j, 1), fwd_sem, dn_dev).start()
    for i in range(hb):
        q_give(i).start()
    for j in range(CP):
        share(chunk_slot(core, j))

    def hand_over(s):
        return pltpu.make_async_remote_copy(
            src_ref=kv.at[s, 0:2], dst_ref=kv.at[s + 1, 2:4], send_sem=sib_sem, recv_sem=recv_sem.at[s + 1, 2],
            device_id=sib_dev, device_id_type=MESH)

    def take(s):
        arrived((s, 0))
        arrived((s, 1))
        hand_over(s).start()
        forward(s)

    def transit(s):
        @pl.when(s < n_transit)
        def _():
            slot = (jnp.minimum(transit0 + s, n_pos - 1), 1)
            arrived(slot)
            send(slot, slot, fwd_sem, dn_dev).start()

    def forward(s):
        lo = low.astype(jnp.int32)
        p1 = s + lo * s
        p2 = p1 + lo
        up2 = up_slot(chip + 1, p2 + CP)
        to2 = (jnp.where(low, up2[0], s), jnp.where(low, up2[1], 1))
        dev2 = dev(jnp.where(low, above, below), core)

        @pl.when(p1 + CP < n_up_above)
        def _():
            send((s, 0), up_slot(chip + 1, p1 + CP), fwd_sem, up_dev).start()

        @pl.when(jnp.where(low, p2 + CP < n_up_above, s < n_dn_below))
        def _():
            send((s, 1), to2, fwd_sem, dev2).start()
        transit(s)

    def qk(i, g, c0, nk, slot, off=None):
        k = kv[g, c0:c0 + nk // ch, 0].reshape(nk, d)
        s = lax.dot_general(k, q_s[i], NT, preferred_element_type=jnp.float32)
        if off is not None:
            key = lax.broadcasted_iota(jnp.int32, (nk, rows), 0)
            tok = lax.broadcasted_iota(jnp.int32, (nk, rows), 1) // 2
            s = jnp.where(key - tok <= off, s, -jnp.inf)
        s_s[slot, 0:nk] = s
        mx_s[slot] = jnp.max(s.reshape(nk // 8, 8, rows), axis=0)

    def sm_pv(i, v, c0, nk, slot, first=False):
        m_new = jnp.max(mx_s[slot], axis=0, keepdims=True)
        if first:
            m_new = jnp.broadcast_to(m_new, (8, rows))
        else:
            m_old = m_s[i]
            m_new = jnp.maximum(m_old, m_new)
            alpha = jnp.exp2((m_old - m_new) * scale2)
        m_s[i] = m_new
        p = jnp.exp2((s_s[slot, 0:nk].reshape(nk // 8, 8, rows) - m_new[None]) * scale2)
        l_new = jnp.sum(p, axis=0)
        pv = lax.dot_general(vt_s[v, :, c0 * ch:c0 * ch + nk], p.reshape(nk, rows).astype(jnp.bfloat16), NN,
                             preferred_element_type=jnp.float32)
        if first:
            l_s[i] = l_new
            acc[i] = pv
        else:
            l_s[i] = l_s[i] * alpha + l_new
            acc[i] = (acc[i].reshape(d // 8, 8, rows) * alpha[None]).reshape(d, rows) + pv

    def make_vt(g, v):
        vt_s[v] = kv[g, :, 1].reshape(gk, d).T

    def make_vt_half(g, c0, v, v0):
        vt_s[v, :, v0 * ch:(v0 + 2) * ch] = kv[g, c0:c0 + 2, 1].reshape(2 * ch, d).T

    own_v = 2

    def run(tiles, last=True):
        qk(tiles[0][0], tiles[0][1], 0, tiles[0][2], 0, tiles[0][3])
        for t, (i, g, nk, off, v, first) in enumerate(tiles):
            if t + 1 < len(tiles):
                qk(tiles[t + 1][0], tiles[t + 1][1], 0, tiles[t + 1][2], (t + 1) % 2, tiles[t + 1][3])
            elif not last:
                break
            sm_pv(i, v, 0, nk, t % 2, first)

    def triangle(k, i0):
        for i in range(hb):
            q_s[i0 + i] = qraw[i0 + i].reshape(rows, d)
        for e in range(2):
            make_vt(own0 + 2 * k + e, own_v + 2 * k + e)
        tiles = []
        for i in range(hb):
            for e in range(i // 2 + 1):
                g, v = own0 + 2 * k + e, own_v + 2 * k + e
                if e < i // 2:
                    tiles.append((i0 + i, g, gk, None, v, e == 0))
                elif i % 2 == 0:
                    tiles.append((i0 + i, g, 2 * ch, ch * core, v, e == 0))
                else:
                    tiles.append((i0 + i, g, gk, ch * (3 - core), v, e == 0))
        run(tiles)

    for copy in qloads:
        copy.wait()
    triangle(core, hb)
    for i in range(hb):
        q_give(i).wait_recv()
    for j in range(CP):
        arrived(chunk_slot(sib, j))
    triangle(sib, 0)

    def stage(g, c0, c1, v, v0, before, after):
        nk = (c1 - c0) * ch
        qk(0, g, c0, nk, 0)
        if before is not None:
            sm_pv(*before, 1)
        for i in range(CP - 1):
            qk(i + 1, g, c0, nk, (i + 1) % 2)
            sm_pv(i, v, v0, nk, i % 2)
            after(i)
        return (CP - 1, v, v0, nk)

    nothing = lambda i: None

    @pl.when(n_steps > 0)
    def _():
        take(0)
        make_vt_half(0, 0, 0, 0)
        sm_pv(*stage(0, 0, 2, 0, 0, None, nothing), 1)

    run([(hb * core + i, own0 + e, gk, None, own_v + e, False) for e in range(2) for i in range(hb)], last=False)

    def before(s):
        first = s == 1
        return (jnp.where(first, hb * core + hb - 1, CP - 1), jnp.where(first, own_v + 1, 1 - lax.rem(s, 2)), 0, gk)

    def step(s, carry):
        hand_over(s - 1).wait_recv()
        take(s)
        v = lax.rem(s, 2)
        make_vt(s, v)
        stage(s, 0, 4, v, 0, before(s), nothing)
        return carry

    lax.fori_loop(1, n_steps - 1, step, 0)

    def o_give(i):
        return pltpu.make_async_remote_copy(
            src_ref=out.at[CP + i], dst_ref=out.at[block_row(core, i)], send_sem=osend_sem.at[i],
            recv_sem=orecv_sem.at[i], device_id=sib_dev, device_id_type=MESH)

    def o_take(i):
        return pltpu.make_async_remote_copy(
            src_ref=out.at[CP + i], dst_ref=out.at[block_row(sib, i)], send_sem=osend_sem.at[i],
            recv_sem=orecv_sem.at[i], device_id=sib_dev, device_id_type=MESH)

    def finish(i):
        inv = 1.0 / jnp.sum(l_s[i], axis=0, keepdims=True)
        o = (acc[i] * inv).astype(jnp.bfloat16).T.reshape(ch, rows // ch, d)
        out[CP + i if i < hb else block_row(core, i)] = o

    def finish_send(i):
        finish(i)
        if i == hb:
            for k in range(hb):
                o_give(k).start()

    @pl.when(n_steps > 0)
    def _():
        s = n_steps - 1
        v = lax.rem(s, 2)
        hand_over(s - 1).wait_recv()
        make_vt_half(s, 2, v, 0)
        last = stage(s, 2, 4, v, 0, before(s), nothing)
        take(s)
        make_vt_half(s, 0, v, 2)
        last = stage(s, 0, 2, v, 2, last, nothing)
        hand_over(s).wait_recv()
        make_vt_half(s + 1, 2, 1 - v, 0)
        last = stage(s + 1, 2, 4, 1 - v, 0, last, finish_send)
        sm_pv(*last, 1)
        finish_send(CP - 1)

    @pl.when(n_steps == 0)
    def _():
        sm_pv(hb * core + hb - 1, own_v + 1, 0, gk, 1)
        for i in range(CP):
            finish_send(i)

    def rest(s, carry):
        transit(s)
        return carry

    lax.fori_loop(n_steps, jnp.maximum(n_steps, n_transit), rest, 0)

    def drain(count, sem):
        def one(i, carry):
            send((own0, 0), (own0, 0), sem, sib_dev).wait_send()
            return carry
        lax.fori_loop(0, count, one, 0)

    own_up = jnp.minimum(n_up_above, CP)
    own_dn = jnp.clip(dn_top - first_dn, 0, CP)
    drain(own_up + jnp.clip(n_up_above - CP, 0, n_up) + own_dn + n_dn_below + n_transit, fwd_sem)
    drain(CP + 2 * n_steps, sib_sem)
    for i in range(hb):
        q_give(i).wait_send()
        o_give(i).wait_send()
        o_take(i).wait_recv()


def store_kernel(o_ref, out_hbm, sem):
    copy = pltpu.make_async_copy(o_ref.at[0:out_hbm.shape[0]], out_hbm, sem)
    copy.start()
    copy.wait()


def solution(mesh):
    n = mesh.shape["ctx"] // 2
    seq_spec = P("data", "ctx", None, None)

    def local_attention(queries, key_rows, value_rows):
        n_batch, chunk_len, n_heads, head_dim = queries.shape
        ch = chunk_len // CP
        rows = ch * n_heads
        n_pos = CP * (n - 1) // 2
        bf16, f32 = jnp.bfloat16, jnp.float32
        hbm = pl.BlockSpec(memory_space=pltpu.HBM)
        dma = pltpu.SemaphoreType.DMA
        out = pl.pallas_call(
            functools.partial(kernel, n, math.log2(math.e) / math.sqrt(head_dim)),
            out_shape=pltpu.VMEM((CP + CP // 2, ch, n_heads, head_dim), bf16),
            in_specs=[hbm, hbm, hbm],
            out_specs=pl.BlockSpec(memory_space=pltpu.VMEM),
            scratch_shapes=[
                pltpu.VMEM((n_pos + 5, 4, 2, ch, head_dim), bf16),
                pltpu.VMEM((CP, ch, n_heads, head_dim), bf16),
                pltpu.VMEM((CP, rows, head_dim), bf16),
                pltpu.VMEM((CP, head_dim, rows), f32),
                pltpu.VMEM((CP, 8, rows), f32),
                pltpu.VMEM((CP, 8, rows), f32),
                pltpu.VMEM((2, 4 * ch, rows), f32),
                pltpu.VMEM((2, 8, rows), f32),
                pltpu.VMEM((6, head_dim, 4 * ch), bf16),
                dma((CP, 2)), dma((CP // 2,)), dma((n_pos + 5, 4)), dma((CP // 2,)), dma((CP // 2,)),
                dma, dma, dma((CP // 2,)), dma((CP // 2,)),
            ],
            compiler_params=pltpu.CompilerParams(
                collective_id=0, has_side_effects=True, vmem_limit_bytes=55 * 1024 * 1024),
            name="attention",
        )(queries.reshape(CP, ch, n_heads, head_dim), key_rows.reshape(CP, ch, head_dim),
          value_rows.reshape(CP, ch, head_dim))
        out = pl.pallas_call(
            store_kernel,
            out_shape=jax.ShapeDtypeStruct((CP, ch, n_heads, head_dim), bf16),
            in_specs=[pl.BlockSpec(memory_space=pltpu.VMEM)],
            out_specs=hbm,
            scratch_shapes=[dma],
            name="store",
        )(pltpu.with_memory_space_constraint(out, pltpu.VMEM))
        return out.reshape(queries.shape)

    return jax.shard_map(local_attention, mesh=mesh, in_specs=(seq_spec, seq_spec, seq_spec),
                         out_specs=seq_spec, check_vma=False)
```

```python
import functools
import math

import jax
import jax.numpy as jnp
from jax import lax
from jax.experimental import pallas as pl
from jax.experimental.pallas import tpu as pltpu
from jax.sharding import PartitionSpec as P

MESH = pl.DeviceIdType.MESH
CP = 8
EXTRA = 2
HALVES = 12
NT = (((1,), (1,)), ((), ()))
NN = (((1,), (0,)), ((), ()))


def kernel(n, scale2, q_hbm, k_hbm, v_hbm, out,
           kv, qraw, q_s, acc, m_s, l_s, s_s, s_left, mx_s, vt_s,
           load_sem, qload_sem, recv_sem, piece_sem, qrecv_sem, orecv_sem,
           fwd_sem, sib_sem, qsend_sem, osend_sem):
    me = lax.axis_index("ctx")
    chip, core = me // 2, me % 2
    sib = 1 - core
    half = n // 2
    hb = CP // 2
    n_pos = CP * (n - 1) // 2
    own0 = n_pos + 1
    ch = k_hbm.shape[1]
    d = k_hbm.shape[2]
    rows = q_s.shape[1]
    gk = 4 * ch

    def dev(c, k):
        return {"ctx": c * 2 + k}

    sib_dev = dev(chip, sib)
    above = lax.rem(chip + 1, n)
    below = lax.rem(chip + n - 1, n)
    up_dev, dn_dev = dev(above, core), dev(below, core)
    low = chip < half

    def extra(c):
        return jnp.where(c == n - 1, 0, EXTRA)

    def up_count(c):
        return jnp.where(c < half, c * CP, c * hb + extra(c))

    def up_slot(c, u):
        lo = c < half
        over = jnp.logical_and(jnp.logical_not(lo), u >= c * hb)
        row = jnp.where(lo, u // 2, jnp.where(over, u - extra(c), u))
        return row, jnp.where(lo, u % 2, over.astype(jnp.int32))

    dn_top = n_pos - extra(n - 1)
    n_up = up_count(chip)
    n_up_above = jnp.where(chip + 1 < n, up_count(chip + 1), 0)
    n_dn_below = jnp.where(chip - 1 < half, 0, (chip - 1) * hb - extra(chip - 1))
    n_steps = chip * hb
    transit0 = CP * (chip + 1)
    n_transit = jnp.where(low, jnp.maximum(dn_top - transit0, 0), 0)

    def chunk_slot(k, j):
        jj = k * CP + j
        return own0 + jj // 4, jj % 4

    def block_row(k, i):
        return 2 * (i % hb) + lax.rem(k + i, 2)

    def send(slot_from, slot_to, sem, device):
        return pltpu.make_async_remote_copy(
            src_ref=kv.at[slot_from[0], slot_from[1]], dst_ref=kv.at[slot_to[0], slot_to[1]],
            send_sem=sem, recv_sem=recv_sem.at[slot_to[0], slot_to[1]],
            device_id=device, device_id_type=MESH)

    def arrived(slot):
        send(slot, slot, sib_sem, sib_dev).wait_recv()

    def load_start(j):
        a, b = chunk_slot(core, j)
        pltpu.make_async_copy(k_hbm.at[j], kv.at[a, b, 0], load_sem.at[j]).start()
        pltpu.make_async_copy(v_hbm.at[j], kv.at[a, b, 1], load_sem.at[j]).start()

    def load_wait(j):
        a, b = chunk_slot(core, j)
        pltpu.make_async_copy(kv.at[a, b], kv.at[a, b], load_sem.at[j]).wait()

    for j in reversed(range(CP)):
        load_start(j)
    qloads = [pltpu.make_async_copy(q_hbm.at[block_row(core, hb + i)], qraw.at[hb + i], qload_sem.at[i])
              for i in range(hb)]
    for copy in qloads:
        copy.start()

    barrier = pltpu.get_barrier_semaphore()
    for device in (sib_dev, up_dev, dn_dev):
        pl.semaphore_signal(barrier, inc=1, device_id=device, device_id_type=MESH)
    pl.semaphore_wait(barrier, 3)

    def q_give(i):
        return pltpu.make_async_remote_copy(
            src_ref=q_hbm.at[block_row(sib, i)], dst_ref=qraw.at[i], send_sem=qsend_sem, recv_sem=qrecv_sem,
            device_id=sib_dev, device_id_type=MESH)

    def q_all():
        return pltpu.make_async_remote_copy(
            src_ref=qraw.at[0:hb], dst_ref=qraw.at[0:hb], send_sem=qsend_sem, recv_sem=qrecv_sem,
            device_id=sib_dev, device_id_type=MESH)

    def piece_give():
        piece = kv.at[pl.ds(own0 + 2 * core, 2)]
        return pltpu.make_async_remote_copy(
            src_ref=piece, dst_ref=piece, send_sem=sib_sem, recv_sem=piece_sem, device_id=sib_dev, device_id_type=MESH)

    first_dn = chip * CP
    for u in range(CP):
        j = CP - 1 - u
        load_wait(j)

        @pl.when(u < n_up_above)
        def _():
            send(chunk_slot(core, j), up_slot(chip + 1, u), fwd_sem, up_dev).start()
    for j in range(CP):
        @pl.when(first_dn + j < dn_top)
        def _():
            send(chunk_slot(core, j), (first_dn + j, 1), fwd_sem, dn_dev).start()
    for i in range(hb):
        q_give(i).start()
    piece_give().start()

    def hand_over(s):
        return pltpu.make_async_remote_copy(
            src_ref=kv.at[s, 0:2], dst_ref=kv.at[s + 1, 2:4], send_sem=sib_sem, recv_sem=recv_sem.at[s + 1, 2],
            device_id=sib_dev, device_id_type=MESH)

    def take(s):
        arrived((s, 0))
        arrived((s, 1))
        hand_over(s).start()
        forward(s)

    def transit(s):
        @pl.when(s < n_transit)
        def _():
            slot = (jnp.minimum(transit0 + s, n_pos - 1), 1)
            arrived(slot)
            send(slot, slot, fwd_sem, dn_dev).start()

    def forward(s):
        lo = low.astype(jnp.int32)
        p1 = s + lo * s
        p2 = p1 + lo
        up2 = up_slot(chip + 1, p2 + CP)
        to2 = (jnp.where(low, up2[0], s), jnp.where(low, up2[1], 1))
        dev2 = dev(jnp.where(low, above, below), core)

        @pl.when(p1 + CP < n_up_above)
        def _():
            send((s, 0), up_slot(chip + 1, p1 + CP), fwd_sem, up_dev).start()

        @pl.when(jnp.where(low, p2 + CP < n_up_above, s < n_dn_below))
        def _():
            send((s, 1), to2, fwd_sem, dev2).start()
        transit(s)

    def score_ref(slot, nk):
        return s_left if slot == 2 else s_s.at[slot, pl.ds(0, nk)]

    def qk(i, g, c0, nk, slot, off=None):
        k = kv[g, c0:c0 + nk // ch, 0].reshape(nk, d)
        s = lax.dot_general(k, q_s[i], NT, preferred_element_type=jnp.float32)
        if off is not None:
            key = lax.broadcasted_iota(jnp.int32, (nk, rows), 0)
            tok = lax.broadcasted_iota(jnp.int32, (nk, rows), 1) // 2
            s = jnp.where(key - tok <= off, s, -jnp.inf)
        score_ref(slot, nk)[...] = s
        mx_s[slot] = jnp.max(s.reshape(nk // 8, 8, rows), axis=0)

    def sm_pv(i, v, c0, nk, slot, first=False, final=None):
        m_new = jnp.max(mx_s[slot], axis=0, keepdims=True)
        if first:
            m_new = jnp.broadcast_to(m_new, (8, rows))
        else:
            m_old = m_s[i]
            m_new = jnp.maximum(m_old, m_new)
            alpha = jnp.exp2((m_old - m_new) * scale2)
        if final is None:
            m_s[i] = m_new
        p = jnp.exp2((score_ref(slot, nk)[...].reshape(nk // 8, 8, rows) - m_new[None]) * scale2)
        l_new = jnp.sum(p, axis=0)
        pv = lax.dot_general(vt_s[v, :, c0 * ch:c0 * ch + nk], p.reshape(nk, rows).astype(jnp.bfloat16), NN,
                             preferred_element_type=jnp.float32)
        if first:
            l_s[i] = l_new
            acc[i] = pv
            return
        l_new = l_s[i] * alpha + l_new
        o = (acc[i].reshape(d // 8, 8, rows) * alpha[None]).reshape(d, rows) + pv
        if final is None:
            l_s[i] = l_new
            acc[i] = o
        else:
            final(i, o, l_new)

    def make_vt(g, v):
        vt_s[v] = kv[g, :, 1].reshape(gk, d).T

    def make_vt_half(g, c0, v, v0):
        vt_s[v, :, v0 * ch:(v0 + 2) * ch] = kv[g, c0:c0 + 2, 1].reshape(2 * ch, d).T

    own_v = 2

    def run(tiles, last=True):
        def slot(t):
            return 2 if t == len(tiles) - 1 and not last else t % 2

        def scores(t):
            i, g, c0, nk, off, v, first = tiles[t]
            qk(i, g, c0, nk, slot(t), off)

        scores(0)
        for t, (i, g, c0, nk, off, v, first) in enumerate(tiles):
            if t + 1 < len(tiles):
                scores(t + 1)
            elif not last:
                break
            sm_pv(i, v, c0, nk, slot(t), first)

    def triangle(k, i0):
        for i in range(hb):
            q_s[i0 + i] = qraw[i0 + i].reshape(rows, d)
        for e in range(2):
            make_vt(own0 + 2 * k + e, own_v + 2 * k + e)
        tiles = []
        for i in range(hb):
            for e in range(i // 2 + 1):
                g, v = own0 + 2 * k + e, own_v + 2 * k + e
                if e < i // 2:
                    tiles.append((i0 + i, g, 0, gk, None, v, e == 0))
                elif i % 2 == 0:
                    tiles.append((i0 + i, g, 0, 2 * ch, ch * core, v, e == 0))
                else:
                    tiles.append((i0 + i, g, 0, gk, ch * (3 - core), v, e == 0))
        run(tiles)

    for copy in qloads:
        copy.wait()
    triangle(core, hb)
    q_all().wait_recv()
    piece_give().wait_recv()
    triangle(sib, 0)

    def stage(g, c0, c1, v, v0, before, leave, final=None):
        nk = (c1 - c0) * ch
        tiles = [(i, c0, nk, v0) for i in range(CP)]
        if leave and c1 - c0 > 2:
            tiles[-1:] = [(CP - 1, c0, 2 * ch, v0), (CP - 1, c0 + 2, 2 * ch, v0 + 2)]
        slots = [t % 2 for t in range(len(tiles))]
        if leave:
            slots[-1] = 2
        for t, (i, c, k, w) in enumerate(tiles):
            qk(i, g, c, k, slots[t])
            if t > 0:
                j, _, k0, w0 = tiles[t - 1]
                sm_pv(j, v, w0, k0, slots[t - 1], final=final)
                if final is not None and t == hb + 1:
                    give_all()
            elif before is not None:
                sm_pv(*before)
        i, _, k, w = tiles[-1]
        return (i, v, w, k, slots[-1])

    @pl.when(n_steps > 0)
    def _():
        take(0)
        make_vt_half(0, 0, 0, 0)
        sm_pv(*stage(0, 0, 2, 0, 0, None, False))

    upper = [(hb * core + i, own0 + e, 0, gk, None, own_v + e, False) for e in range(2) for i in range(hb)]
    i, g, _, _, _, v, _ = upper[-1]
    upper[-1:] = [(i, g, c, 2 * ch, None, v, False) for c in (0, 2)]
    run(upper, last=False)

    def before(s):
        first = s == 1
        return (jnp.where(first, hb * core + hb - 1, CP - 1), jnp.where(first, own_v + 1, 1 - lax.rem(s, 2)), 2, 2 * ch, 2)

    def step(s, carry):
        hand_over(s - 1).wait_recv()
        take(s)
        v = lax.rem(s, 2)
        make_vt(s, v)
        stage(s, 0, 4, v, 0, before(s), True)
        return carry

    def half_steps(s, carry):
        hand_over(s - 1).wait_recv()
        v = lax.rem(s, 2)
        make_vt_half(s, 2, v, 0)
        left = stage(s, 2, 4, v, 0, before(s), False)
        take(s)
        make_vt_half(s, 0, v, 2)
        stage(s, 0, 2, v, 2, left, True)
        return carry

    n_merged = jnp.maximum(n_steps - HALVES, 1)
    lax.fori_loop(1, n_merged, step, 0)
    lax.fori_loop(n_merged, n_steps, half_steps, 0)

    def o_give(i):
        return pltpu.make_async_remote_copy(
            src_ref=out.at[CP + i], dst_ref=out.at[block_row(core, i)], send_sem=osend_sem, recv_sem=orecv_sem,
            device_id=sib_dev, device_id_type=MESH)

    def o_all():
        return pltpu.make_async_remote_copy(
            src_ref=out.at[CP:CP + hb], dst_ref=out.at[CP:CP + hb], send_sem=osend_sem, recv_sem=orecv_sem,
            device_id=sib_dev, device_id_type=MESH)

    def give_all():
        for i in range(hb):
            o_give(i).start()

    def store_rows(i, o, l):
        inv = 1.0 / jnp.sum(l, axis=0, keepdims=True)
        out[jnp.where(i < hb, CP + i, block_row(core, i))] = (o * inv).astype(jnp.bfloat16).T.reshape(ch, rows // ch, d)

    @pl.when(n_steps > 0)
    def _():
        s = n_steps - 1
        v = 1 - lax.rem(s, 2)
        hand_over(s).wait_recv()
        make_vt_half(s + 1, 2, v, 0)
        sm_pv(*stage(s + 1, 2, 4, v, 0, before(s + 1), False, final=store_rows), final=store_rows)

    @pl.when(n_steps == 0)
    def _():
        sm_pv(hb * core + hb - 1, own_v + 1, 2, 2 * ch, 2)

        def store_block(i, carry):
            store_rows(i, acc[i], l_s[i])
            return carry
        lax.fori_loop(0, CP, store_block, 0)
        give_all()

    def rest(s, carry):
        transit(s)
        return carry

    lax.fori_loop(n_steps, jnp.maximum(n_steps, n_transit), rest, 0)

    def drain(count, sem):
        def rows_of_four(i, carry):
            pltpu.make_async_remote_copy(
                src_ref=kv.at[0], dst_ref=kv.at[0], send_sem=sem, recv_sem=piece_sem, device_id=sib_dev,
                device_id_type=MESH).wait_send()
            return carry

        def single(i, carry):
            send((0, 0), (0, 0), sem, sib_dev).wait_send()
            return carry
        lax.fori_loop(0, count // 4, rows_of_four, 0)
        lax.fori_loop(0, count % 4, single, 0)

    own_up = jnp.minimum(n_up_above, CP)
    own_dn = jnp.clip(dn_top - first_dn, 0, CP)
    drain(own_up + jnp.clip(n_up_above - CP, 0, n_up) + own_dn + n_dn_below + n_transit, fwd_sem)
    drain(CP + 2 * n_steps, sib_sem)
    q_all().wait_send()
    o_all().wait_send()
    o_all().wait_recv()


def store_kernel(o_ref, out_hbm, sem):
    copy = pltpu.make_async_copy(o_ref.at[0:out_hbm.shape[0]], out_hbm, sem)
    copy.start()
    copy.wait()


def solution(mesh):
    n = mesh.shape["ctx"] // 2
    seq_spec = P("data", "ctx", None, None)

    def local_attention(queries, key_rows, value_rows):
        n_batch, chunk_len, n_heads, head_dim = queries.shape
        ch = chunk_len // CP
        rows = ch * n_heads
        n_pos = CP * (n - 1) // 2
        bf16, f32 = jnp.bfloat16, jnp.float32
        hbm = pl.BlockSpec(memory_space=pltpu.HBM)
        dma = pltpu.SemaphoreType.DMA
        out = pl.pallas_call(
            functools.partial(kernel, n, math.log2(math.e) / math.sqrt(head_dim)),
            out_shape=pltpu.VMEM((CP + CP // 2, ch, n_heads, head_dim), bf16),
            in_specs=[hbm, hbm, hbm],
            out_specs=pl.BlockSpec(memory_space=pltpu.VMEM),
            scratch_shapes=[
                pltpu.VMEM((n_pos + 5, 4, 2, ch, head_dim), bf16),
                pltpu.VMEM((CP, ch, n_heads, head_dim), bf16),
                pltpu.VMEM((CP, rows, head_dim), bf16),
                pltpu.VMEM((CP, head_dim, rows), f32),
                pltpu.VMEM((CP, 8, rows), f32),
                pltpu.VMEM((CP, 8, rows), f32),
                pltpu.VMEM((2, 4 * ch, rows), f32),
                pltpu.VMEM((2 * ch, rows), f32),
                pltpu.VMEM((3, 8, rows), f32),
                pltpu.VMEM((6, head_dim, 4 * ch), bf16),
                dma((CP,)), dma((CP // 2,)), dma((n_pos + 1, 3)), dma, dma, dma, dma, dma, dma, dma,
            ],
            compiler_params=pltpu.CompilerParams(
                collective_id=0, has_side_effects=True, vmem_limit_bytes=58 * 1024 * 1024),
            name="attention",
        )(queries.reshape(CP, ch, n_heads, head_dim), key_rows.reshape(CP, ch, head_dim),
          value_rows.reshape(CP, ch, head_dim))
        out = pl.pallas_call(
            store_kernel,
            out_shape=jax.ShapeDtypeStruct((CP, ch, n_heads, head_dim), bf16),
            in_specs=[pl.BlockSpec(memory_space=pltpu.VMEM)],
            out_specs=hbm,
            scratch_shapes=[dma],
            name="store",
        )(pltpu.with_memory_space_constraint(out, pltpu.VMEM))
        return out.reshape(queries.shape)

    return jax.shard_map(local_attention, mesh=mesh, in_specs=(seq_spec, seq_spec, seq_spec),
                         out_specs=seq_spec, check_vma=False)
```

```python
import functools
import math

import jax
import jax.numpy as jnp
from jax import lax
from jax.experimental import pallas as pl
from jax.experimental.pallas import tpu as pltpu
from jax.sharding import PartitionSpec as P

MESH = pl.DeviceIdType.MESH
CP = 8
EXTRA = 2
HALVES = 19
NT = (((1,), (1,)), ((), ()))
NN = (((1,), (0,)), ((), ()))


def kernel(n, scale2, q_hbm, k_hbm, v_hbm, out,
           kv, qraw, q_s, acc, m_s, l_s, s_s, s_left, mx_s, vt_s,
           load_sem, qload_sem, recv_sem, piece_sem, qrecv_sem, orecv_sem,
           fwd_sem, sib_sem, qsend_sem, osend_sem):
    me = lax.axis_index("ctx")
    chip, core = me // 2, me % 2
    sib = 1 - core
    half = n // 2
    hb = CP // 2
    n_pos = CP * (n - 1) // 2
    own0 = n_pos + 1
    ch = k_hbm.shape[1]
    d = k_hbm.shape[2]
    rows = q_s.shape[1]
    gk = 4 * ch

    def dev(c, k):
        return {"ctx": c * 2 + k}

    sib_dev = dev(chip, sib)
    above = lax.rem(chip + 1, n)
    below = lax.rem(chip + n - 1, n)
    up_dev, dn_dev = dev(above, core), dev(below, core)
    low = chip < half

    def extra(c):
        return jnp.where(c == n - 1, 0, EXTRA)

    def up_count(c):
        return jnp.where(c < half, c * CP, c * hb + extra(c))

    def up_slot(c, u):
        lo = c < half
        over = jnp.logical_and(jnp.logical_not(lo), u >= c * hb)
        row = jnp.where(lo, u // 2, jnp.where(over, u - extra(c), u))
        return row, jnp.where(lo, u % 2, over.astype(jnp.int32))

    dn_top = n_pos - extra(n - 1)
    n_up = up_count(chip)
    n_up_above = jnp.where(chip + 1 < n, up_count(chip + 1), 0)
    n_dn_below = jnp.where(chip - 1 < half, 0, (chip - 1) * hb - extra(chip - 1))
    n_steps = chip * hb
    transit0 = CP * (chip + 1)
    n_transit = jnp.where(low, jnp.maximum(dn_top - transit0, 0), 0)

    def chunk_slot(k, j):
        jj = k * CP + j
        return own0 + jj // 4, jj % 4

    def block_row(k, i):
        return 2 * (i % hb) + lax.rem(k + i, 2)

    def send(slot_from, slot_to, sem, device):
        return pltpu.make_async_remote_copy(
            src_ref=kv.at[slot_from[0], slot_from[1]], dst_ref=kv.at[slot_to[0], slot_to[1]],
            send_sem=sem, recv_sem=recv_sem.at[slot_to[0], 0],
            device_id=device, device_id_type=MESH)

    barrier = pltpu.get_barrier_semaphore()
    for device in (sib_dev, up_dev, dn_dev):
        pl.semaphore_signal(barrier, inc=1, device_id=device, device_id_type=MESH)

    def load_start(j):
        a, b = chunk_slot(core, j)
        pltpu.make_async_copy(k_hbm.at[j], kv.at[a, b, 0], load_sem.at[j]).start()
        pltpu.make_async_copy(v_hbm.at[j], kv.at[a, b, 1], load_sem.at[j]).start()

    def load_wait(j):
        a, b = chunk_slot(core, j)
        pltpu.make_async_copy(kv.at[a, b], kv.at[a, b], load_sem.at[j]).wait()

    for j in range(hb):
        load_start(CP - 1 - j)
        load_start(j)
    qloads = [pltpu.make_async_copy(q_hbm.at[block_row(core, hb + i)], qraw.at[hb + i], qload_sem.at[i])
              for i in range(hb)]
    for copy in qloads:
        copy.start()

    pl.semaphore_wait(barrier, 3)

    def q_give(i):
        return pltpu.make_async_remote_copy(
            src_ref=q_hbm.at[block_row(sib, i)], dst_ref=qraw.at[i], send_sem=qsend_sem, recv_sem=qrecv_sem,
            device_id=sib_dev, device_id_type=MESH)

    def q_all():
        return pltpu.make_async_remote_copy(
            src_ref=qraw.at[0:hb], dst_ref=qraw.at[0:hb], send_sem=qsend_sem, recv_sem=qrecv_sem,
            device_id=sib_dev, device_id_type=MESH)

    def piece_give():
        piece = kv.at[pl.ds(own0 + 2 * core, 2)]
        return pltpu.make_async_remote_copy(
            src_ref=piece, dst_ref=piece, send_sem=sib_sem, recv_sem=piece_sem, device_id=sib_dev, device_id_type=MESH)

    first_dn = chip * CP
    for u in range(CP):
        if u < hb:
            load_wait(CP - 1 - u)
            load_wait(u)

        @pl.when(first_dn + u < dn_top)
        def _():
            send(chunk_slot(core, u), (first_dn + u, 1), fwd_sem, dn_dev).start()

        @pl.when(u < n_up_above)
        def _():
            send(chunk_slot(core, CP - 1 - u), up_slot(chip + 1, u), fwd_sem, up_dev).start()
    for i in range(hb):
        q_give(i).start()
    piece_give().start()

    def hand_over(s):
        return pltpu.make_async_remote_copy(
            src_ref=kv.at[s, 0:2], dst_ref=kv.at[s + 1, 2:4], send_sem=sib_sem, recv_sem=recv_sem.at[s + 1, 1],
            device_id=sib_dev, device_id_type=MESH)

    def take(s):
        pltpu.make_async_remote_copy(
            src_ref=kv.at[s, 0:2], dst_ref=kv.at[s, 0:2], send_sem=sib_sem, recv_sem=recv_sem.at[s, 0],
            device_id=sib_dev, device_id_type=MESH).wait_recv()
        hand_over(s).start()
        forward(s)

    def transit(s):
        @pl.when(s < n_transit)
        def _():
            slot = (jnp.minimum(transit0 + s, n_pos - 1), 1)
            send(slot, slot, fwd_sem, dn_dev).wait_recv()
            send(slot, slot, fwd_sem, dn_dev).start()

    def forward(s):
        lo = low.astype(jnp.int32)
        p1 = s + lo * s
        p2 = p1 + lo
        up2 = up_slot(chip + 1, p2 + CP)
        to2 = (jnp.where(low, up2[0], s), jnp.where(low, up2[1], 1))
        dev2 = dev(jnp.where(low, above, below), core)

        @pl.when(p1 + CP < n_up_above)
        def _():
            send((s, 0), up_slot(chip + 1, p1 + CP), fwd_sem, up_dev).start()

        @pl.when(jnp.where(low, p2 + CP < n_up_above, s < n_dn_below))
        def _():
            send((s, 1), to2, fwd_sem, dev2).start()
        transit(s)

    def score_ref(slot, nk):
        return s_left if slot == 2 else s_s.at[slot, pl.ds(0, nk)]

    def qk(i, g, c0, nk, slot, off=None):
        k = kv[g, c0:c0 + nk // ch, 0].reshape(nk, d)
        s = lax.dot_general(k, q_s[i], NT, preferred_element_type=jnp.float32)
        if off is not None:
            key = lax.broadcasted_iota(jnp.int32, (nk, rows), 0)
            tok = lax.broadcasted_iota(jnp.int32, (nk, rows), 1) // 2
            s = jnp.where(key - tok <= off, s, -jnp.inf)
        score_ref(slot, nk)[...] = s
        mx_s[slot] = jnp.max(s.reshape(nk // 8, 8, rows), axis=0)

    def sm_pv(i, v, c0, nk, slot, first=False, final=None):
        m_new = jnp.max(mx_s[slot], axis=0, keepdims=True)
        if first:
            m_new = jnp.broadcast_to(m_new, (8, rows))
        else:
            m_old = m_s[i]
            m_new = jnp.maximum(m_old, m_new)
            alpha = jnp.exp2((m_old - m_new) * scale2)
        if final is None:
            m_s[i] = m_new
        p = jnp.exp2((score_ref(slot, nk)[...].reshape(nk // 8, 8, rows) - m_new[None]) * scale2)
        l_new = jnp.sum(p, axis=0)
        pv = lax.dot_general(vt_s[v, :, c0 * ch:c0 * ch + nk], p.reshape(nk, rows).astype(jnp.bfloat16), NN,
                             preferred_element_type=jnp.float32)
        if first:
            l_s[i] = l_new
            acc[i] = pv
            return
        l_new = l_s[i] * alpha + l_new
        o = (acc[i].reshape(d // 8, 8, rows) * alpha[None]).reshape(d, rows) + pv
        if final is None:
            l_s[i] = l_new
            acc[i] = o
        else:
            final(i, o, l_new)

    def make_vt(g, v):
        vt_s[v] = kv[g, :, 1].reshape(gk, d).T

    def make_vt_half(g, c0, v, v0):
        vt_s[v, :, v0 * ch:(v0 + 2) * ch] = kv[g, c0:c0 + 2, 1].reshape(2 * ch, d).T

    own_v = 2

    def run(tiles, last=True):
        def slot(t):
            return 2 if t == len(tiles) - 1 and not last else t % 2

        def scores(t):
            i, g, c0, nk, off, v, first = tiles[t]
            qk(i, g, c0, nk, slot(t), off)

        scores(0)
        for t, (i, g, c0, nk, off, v, first) in enumerate(tiles):
            if t + 1 < len(tiles):
                scores(t + 1)
            elif not last:
                break
            sm_pv(i, v, c0, nk, slot(t), first)

    def triangle(k, i0):
        for i in range(hb):
            q_s[i0 + i] = qraw[i0 + i].reshape(rows, d)
        for e in range(2):
            make_vt(own0 + 2 * k + e, own_v + 2 * k + e)
        tiles = []
        for i in range(hb):
            for e in range(i // 2 + 1):
                g, v = own0 + 2 * k + e, own_v + 2 * k + e
                if e < i // 2:
                    tiles.append((i0 + i, g, 0, gk, None, v, e == 0))
                elif i % 2 == 0:
                    tiles.append((i0 + i, g, 0, 2 * ch, ch * core, v, e == 0))
                else:
                    tiles.append((i0 + i, g, 0, gk, ch * (3 - core), v, e == 0))
        run(tiles)

    for copy in qloads:
        copy.wait()
    triangle(core, hb)
    q_all().wait_recv()
    piece_give().wait_recv()
    triangle(sib, 0)

    def stage(g, c0, c1, v, v0, before, leave, final=None):
        nk = (c1 - c0) * ch
        tiles = [(i, c0, nk, v0) for i in range(CP)]
        if leave and c1 - c0 > 2:
            tiles[-1:] = [(CP - 1, c0, 2 * ch, v0), (CP - 1, c0 + 2, 2 * ch, v0 + 2)]
        slots = [t % 2 for t in range(len(tiles))]
        if leave:
            slots[-1] = 2
        for t, (i, c, k, w) in enumerate(tiles):
            qk(i, g, c, k, slots[t])
            if t > 0:
                j, _, k0, w0 = tiles[t - 1]
                sm_pv(j, v, w0, k0, slots[t - 1], final=final)
                if final is not None and t == hb:
                    give(range(hb - 1))
                if final is not None and t == hb + 1:
                    give([hb - 1])
            elif before is not None:
                sm_pv(*before)
        i, _, k, w = tiles[-1]
        return (i, v, w, k, slots[-1])

    @pl.when(n_steps > 0)
    def _():
        take(0)
        make_vt_half(0, 0, 0, 0)
        sm_pv(*stage(0, 0, 2, 0, 0, None, False))

    upper = [(hb * core + i, own0 + e, 0, gk, None, own_v + e, False) for e in range(2) for i in range(hb)]
    i, g, _, _, _, v, _ = upper[-1]
    upper[-1:] = [(i, g, c, 2 * ch, None, v, False) for c in (0, 2)]
    run(upper, last=False)

    def before(s):
        first = s == 1
        return (jnp.where(first, hb * core + hb - 1, CP - 1), jnp.where(first, own_v + 1, 1 - lax.rem(s, 2)), 2, 2 * ch, 2)

    def step(s, carry):
        hand_over(s - 1).wait_recv()
        take(s)
        v = lax.rem(s, 2)
        make_vt(s, v)
        stage(s, 0, 4, v, 0, before(s), True)
        return carry

    def half_steps(s, carry):
        hand_over(s - 1).wait_recv()
        v = lax.rem(s, 2)
        make_vt_half(s, 2, v, 0)
        left = stage(s, 2, 4, v, 0, before(s), False)
        take(s)
        make_vt_half(s, 0, v, 2)
        stage(s, 0, 2, v, 2, left, True)
        return carry

    n_merged = jnp.maximum(n_steps - HALVES, 1)
    lax.fori_loop(1, n_merged, step, 0)
    lax.fori_loop(n_merged, n_steps, half_steps, 0)

    def o_give(i):
        return pltpu.make_async_remote_copy(
            src_ref=out.at[CP + i], dst_ref=out.at[block_row(core, i)], send_sem=osend_sem, recv_sem=orecv_sem,
            device_id=sib_dev, device_id_type=MESH)

    def o_all():
        return pltpu.make_async_remote_copy(
            src_ref=out.at[CP:CP + hb], dst_ref=out.at[CP:CP + hb], send_sem=osend_sem, recv_sem=orecv_sem,
            device_id=sib_dev, device_id_type=MESH)

    def give(blocks):
        for i in blocks:
            o_give(i).start()

    def store_rows(i, o, l):
        inv = 1.0 / jnp.sum(l, axis=0, keepdims=True)
        out[jnp.where(i < hb, CP + i, block_row(core, i))] = (o * inv).astype(jnp.bfloat16).T.reshape(ch, rows // ch, d)

    @pl.when(n_steps > 0)
    def _():
        s = n_steps - 1
        v = 1 - lax.rem(s, 2)
        hand_over(s).wait_recv()
        make_vt_half(s + 1, 2, v, 0)
        sm_pv(*stage(s + 1, 2, 4, v, 0, before(s + 1), False, final=store_rows), final=store_rows)

    @pl.when(n_steps == 0)
    def _():
        sm_pv(hb * core + hb - 1, own_v + 1, 2, 2 * ch, 2)

        def store_block(i, carry):
            store_rows(i, acc[i], l_s[i])
            return carry
        lax.fori_loop(0, CP, store_block, 0)
        give(range(hb))

    def rest(s, carry):
        transit(s)
        return carry

    lax.fori_loop(n_steps, jnp.maximum(n_steps, n_transit), rest, 0)

    def drain(count, sem):
        def rows_of_four(i, carry):
            pltpu.make_async_remote_copy(
                src_ref=kv.at[0], dst_ref=kv.at[0], send_sem=sem, recv_sem=piece_sem, device_id=sib_dev,
                device_id_type=MESH).wait_send()
            return carry

        def single(i, carry):
            send((0, 0), (0, 0), sem, sib_dev).wait_send()
            return carry
        lax.fori_loop(0, count // 4, rows_of_four, 0)
        lax.fori_loop(0, count % 4, single, 0)

    own_up = jnp.minimum(n_up_above, CP)
    own_dn = jnp.clip(dn_top - first_dn, 0, CP)
    drain(own_up + jnp.clip(n_up_above - CP, 0, n_up) + own_dn + n_dn_below + n_transit, fwd_sem)
    drain(CP + 2 * n_steps, sib_sem)
    q_all().wait_send()
    o_all().wait_send()
    o_all().wait_recv()


def store_kernel(o_ref, out_hbm, sem):
    copies = [pltpu.make_async_copy(o_ref.at[i], out_hbm.at[i], sem.at[i]) for i in range(out_hbm.shape[0])]
    for copy in copies:
        copy.start()
    for copy in copies:
        copy.wait()


def solution(mesh):
    n = mesh.shape["ctx"] // 2
    seq_spec = P("data", "ctx", None, None)

    def local_attention(queries, key_rows, value_rows):
        n_batch, chunk_len, n_heads, head_dim = queries.shape
        ch = chunk_len // CP
        rows = ch * n_heads
        n_pos = CP * (n - 1) // 2
        bf16, f32 = jnp.bfloat16, jnp.float32
        hbm = pl.BlockSpec(memory_space=pltpu.HBM)
        dma = pltpu.SemaphoreType.DMA
        out = pl.pallas_call(
            functools.partial(kernel, n, math.log2(math.e) / math.sqrt(head_dim)),
            out_shape=pltpu.VMEM((CP + CP // 2, ch, n_heads, head_dim), bf16),
            in_specs=[hbm, hbm, hbm],
            out_specs=pl.BlockSpec(memory_space=pltpu.VMEM),
            scratch_shapes=[
                pltpu.VMEM((n_pos + 5, 4, 2, ch, head_dim), bf16),
                pltpu.VMEM((CP, ch, n_heads, head_dim), bf16),
                pltpu.VMEM((CP, rows, head_dim), bf16),
                pltpu.VMEM((CP, head_dim, rows), f32),
                pltpu.VMEM((CP, 8, rows), f32),
                pltpu.VMEM((CP, 8, rows), f32),
                pltpu.VMEM((2, 4 * ch, rows), f32),
                pltpu.VMEM((2 * ch, rows), f32),
                pltpu.VMEM((3, 8, rows), f32),
                pltpu.VMEM((6, head_dim, 4 * ch), bf16),
                dma((CP,)), dma((CP // 2,)), dma((n_pos + 1, 2)), dma, dma, dma, dma, dma, dma, dma,
            ],
            compiler_params=pltpu.CompilerParams(
                collective_id=0, has_side_effects=True, vmem_limit_bytes=58 * 1024 * 1024),
            name="attention",
        )(queries.reshape(CP, ch, n_heads, head_dim), key_rows.reshape(CP, ch, head_dim),
          value_rows.reshape(CP, ch, head_dim))
        out = pl.pallas_call(
            store_kernel,
            out_shape=jax.ShapeDtypeStruct((CP, ch, n_heads, head_dim), bf16),
            in_specs=[pl.BlockSpec(memory_space=pltpu.VMEM)],
            out_specs=hbm,
            scratch_shapes=[dma((CP,))],
            name="store",
        )(pltpu.with_memory_space_constraint(out, pltpu.VMEM))
        return out.reshape(queries.shape)

    return jax.shard_map(local_attention, mesh=mesh, in_specs=(seq_spec, seq_spec, seq_spec),
                         out_specs=seq_spec, check_vma=False)
```

```python
import functools
import math

import jax
import jax.numpy as jnp
from jax import lax
from jax.experimental import pallas as pl
from jax.experimental.pallas import tpu as pltpu
from jax.sharding import PartitionSpec as P

MESH = pl.DeviceIdType.MESH
CP = 8
EXTRA = 2
HALVES = 22
NT = (((1,), (1,)), ((), ()))
NN = (((1,), (0,)), ((), ()))


def kernel(n, scale2, q_hbm, k_hbm, v_hbm, out,
           kv, qraw, q_s, acc, m_s, l_s, s_s, s_left, mx_s, vt_s,
           load_sem, qload_sem, recv_sem, piece_sem, qrecv_sem, orecv_sem,
           fwd_sem, sib_sem, qsend_sem, osend_sem):
    me = lax.axis_index("ctx")
    chip, core = me // 2, me % 2
    sib = 1 - core
    half = n // 2
    hb = CP // 2
    n_pos = CP * (n - 1) // 2
    own0 = n_pos + 1
    ch = k_hbm.shape[1]
    d = k_hbm.shape[2]
    rows = q_s.shape[1]
    gk = 4 * ch

    def dev(c, k):
        return {"ctx": c * 2 + k}

    sib_dev = dev(chip, sib)
    above = lax.rem(chip + 1, n)
    below = lax.rem(chip + n - 1, n)
    up_dev, dn_dev = dev(above, core), dev(below, core)
    low = chip < half

    def extra(c):
        return jnp.where(c == n - 1, 0, EXTRA)

    def up_count(c):
        return jnp.where(c < half, c * CP, c * hb + extra(c))

    def up_slot(c, u):
        lo = c < half
        over = jnp.logical_and(jnp.logical_not(lo), u >= c * hb)
        row = jnp.where(lo, u // 2, jnp.where(over, u - extra(c), u))
        return row, jnp.where(lo, u % 2, over.astype(jnp.int32))

    dn_top = n_pos - extra(n - 1)
    n_up = up_count(chip)
    n_up_above = jnp.where(chip + 1 < n, up_count(chip + 1), 0)
    n_dn_below = jnp.where(chip - 1 < half, 0, (chip - 1) * hb - extra(chip - 1))
    n_steps = chip * hb
    transit0 = CP * (chip + 1)
    n_transit = jnp.where(low, jnp.maximum(dn_top - transit0, 0), 0)

    def chunk_slot(k, j):
        jj = k * CP + j
        return own0 + jj // 4, jj % 4

    def block_row(k, i):
        return 2 * (i % hb) + lax.rem(k + i, 2)

    def send(slot_from, slot_to, sem, device):
        return pltpu.make_async_remote_copy(
            src_ref=kv.at[slot_from[0], slot_from[1]], dst_ref=kv.at[slot_to[0], slot_to[1]],
            send_sem=sem, recv_sem=recv_sem.at[slot_to[0], 0],
            device_id=device, device_id_type=MESH)

    barrier = pltpu.get_barrier_semaphore()
    for device in (sib_dev, up_dev, dn_dev):
        pl.semaphore_signal(barrier, inc=1, device_id=device, device_id_type=MESH)

    def load_start(j):
        a, b = chunk_slot(core, j)
        pltpu.make_async_copy(k_hbm.at[j], kv.at[a, b, 0], load_sem.at[j]).start()
        pltpu.make_async_copy(v_hbm.at[j], kv.at[a, b, 1], load_sem.at[j]).start()

    def load_wait(j):
        a, b = chunk_slot(core, j)
        pltpu.make_async_copy(kv.at[a, b], kv.at[a, b], load_sem.at[j]).wait()

    for j in range(hb):
        load_start(CP - 1 - j)
        load_start(j)
    qloads = [pltpu.make_async_copy(q_hbm.at[block_row(core, hb + i)], qraw.at[hb + i], qload_sem.at[i])
              for i in range(hb)]
    for copy in qloads:
        copy.start()

    pl.semaphore_wait(barrier, 3)

    def q_give(i):
        return pltpu.make_async_remote_copy(
            src_ref=q_hbm.at[block_row(sib, i)], dst_ref=qraw.at[i], send_sem=qsend_sem, recv_sem=qrecv_sem,
            device_id=sib_dev, device_id_type=MESH)

    def q_all():
        return pltpu.make_async_remote_copy(
            src_ref=qraw.at[0:hb], dst_ref=qraw.at[0:hb], send_sem=qsend_sem, recv_sem=qrecv_sem,
            device_id=sib_dev, device_id_type=MESH)

    def piece_give():
        piece = kv.at[pl.ds(own0 + 2 * core, 2)]
        return pltpu.make_async_remote_copy(
            src_ref=piece, dst_ref=piece, send_sem=sib_sem, recv_sem=piece_sem, device_id=sib_dev, device_id_type=MESH)

    first_dn = chip * CP
    for u in range(CP):
        if u < hb:
            load_wait(CP - 1 - u)
            load_wait(u)

        @pl.when(first_dn + u < dn_top)
        def _():
            send(chunk_slot(core, u), (first_dn + u, 1), fwd_sem, dn_dev).start()

        @pl.when(u < n_up_above)
        def _():
            send(chunk_slot(core, CP - 1 - u), up_slot(chip + 1, u), fwd_sem, up_dev).start()
    for i in range(hb):
        q_give(i).start()
    piece_give().start()

    def hand_over(s):
        return pltpu.make_async_remote_copy(
            src_ref=kv.at[s, 0:2], dst_ref=kv.at[s + 1, 2:4], send_sem=sib_sem, recv_sem=recv_sem.at[s + 1, 1],
            device_id=sib_dev, device_id_type=MESH)

    def take(s):
        pltpu.make_async_remote_copy(
            src_ref=kv.at[s, 0:2], dst_ref=kv.at[s, 0:2], send_sem=sib_sem, recv_sem=recv_sem.at[s, 0],
            device_id=sib_dev, device_id_type=MESH).wait_recv()
        hand_over(s).start()
        forward(s)

    def transit(s):
        @pl.when(s < n_transit)
        def _():
            slot = (jnp.minimum(transit0 + s, n_pos - 1), 1)
            send(slot, slot, fwd_sem, dn_dev).wait_recv()
            send(slot, slot, fwd_sem, dn_dev).start()

    def forward(s):
        lo = low.astype(jnp.int32)
        p1 = s + lo * s
        p2 = p1 + lo
        up2 = up_slot(chip + 1, p2 + CP)
        to2 = (jnp.where(low, up2[0], s), jnp.where(low, up2[1], 1))
        dev2 = dev(jnp.where(low, above, below), core)

        @pl.when(p1 + CP < n_up_above)
        def _():
            send((s, 0), up_slot(chip + 1, p1 + CP), fwd_sem, up_dev).start()

        @pl.when(jnp.where(low, p2 + CP < n_up_above, s < n_dn_below))
        def _():
            send((s, 1), to2, fwd_sem, dev2).start()
        transit(s)

    def score_ref(slot, nk):
        return s_left if slot == 2 else s_s.at[slot, pl.ds(0, nk)]

    def qk(i, g, c0, nk, slot, off=None):
        k = kv[g, c0:c0 + nk // ch, 0].reshape(nk, d)
        s = lax.dot_general(k, q_s[i], NT, preferred_element_type=jnp.float32)
        if off is not None:
            key = lax.broadcasted_iota(jnp.int32, (nk, rows), 0)
            tok = lax.broadcasted_iota(jnp.int32, (nk, rows), 1) // 2
            s = jnp.where(key - tok <= off, s, -jnp.inf)
        score_ref(slot, nk)[...] = s
        mx_s[slot] = jnp.max(s.reshape(nk // 8, 8, rows), axis=0)

    def sm_pv(i, v, c0, nk, slot, first=False, final=None):
        m_new = jnp.max(mx_s[slot], axis=0, keepdims=True)
        if first:
            m_new = jnp.broadcast_to(m_new, (8, rows))
        else:
            m_old = m_s[i]
            m_new = jnp.maximum(m_old, m_new)
            alpha = jnp.exp2((m_old - m_new) * scale2)
        if final is None:
            m_s[i] = m_new
        p = jnp.exp2((score_ref(slot, nk)[...].reshape(nk // 8, 8, rows) - m_new[None]) * scale2)
        l_new = jnp.sum(p, axis=0)
        pv = lax.dot_general(vt_s[v, :, c0 * ch:c0 * ch + nk], p.reshape(nk, rows).astype(jnp.bfloat16), NN,
                             preferred_element_type=jnp.float32)
        if first:
            l_s[i] = l_new
            acc[i] = pv
            return
        l_new = l_s[i] * alpha + l_new
        o = (acc[i].reshape(d // 8, 8, rows) * alpha[None]).reshape(d, rows) + pv
        if final is None:
            l_s[i] = l_new
            acc[i] = o
        else:
            final(i, o, l_new)

    def make_vt(g, v):
        vt_s[v] = kv[g, :, 1].reshape(gk, d).T

    def make_vt_half(g, c0, v, v0):
        vt_s[v, :, v0 * ch:(v0 + 2) * ch] = kv[g, c0:c0 + 2, 1].reshape(2 * ch, d).T

    own_v = 2

    def run(tiles, last=True):
        def slot(t):
            return 2 if t == len(tiles) - 1 and not last else t % 2

        def scores(t):
            i, g, c0, nk, off, v, first = tiles[t]
            qk(i, g, c0, nk, slot(t), off)

        scores(0)
        for t, (i, g, c0, nk, off, v, first) in enumerate(tiles):
            if t + 1 < len(tiles):
                scores(t + 1)
            elif not last:
                break
            sm_pv(i, v, c0, nk, slot(t), first)

    def triangle(k, i0):
        for i in range(hb):
            q_s[i0 + i] = qraw[i0 + i].reshape(rows, d)
        for e in range(2):
            make_vt(own0 + 2 * k + e, own_v + 2 * k + e)
        tiles = []
        for i in range(hb):
            for e in range(i // 2 + 1):
                g, v = own0 + 2 * k + e, own_v + 2 * k + e
                if e < i // 2:
                    tiles.append((i0 + i, g, 0, gk, None, v, e == 0))
                elif i % 2 == 0:
                    tiles.append((i0 + i, g, 0, 2 * ch, ch * core, v, e == 0))
                else:
                    tiles.append((i0 + i, g, 0, gk, ch * (3 - core), v, e == 0))
        run(tiles)

    for copy in qloads:
        copy.wait()
    @pl.when(chip >= 0)
    def _():
        triangle(core, hb)

    @pl.when(chip >= 0)
    def _():
        q_all().wait_recv()
        piece_give().wait_recv()
        triangle(sib, 0)

    def stage(g, c0, c1, v, v0, before, leave, final=None):
        nk = (c1 - c0) * ch
        tiles = [(i, c0, nk, v0) for i in range(CP)]
        if leave and c1 - c0 > 2:
            tiles[-1:] = [(CP - 1, c0, 2 * ch, v0), (CP - 1, c0 + 2, 2 * ch, v0 + 2)]
        slots = [t % 2 for t in range(len(tiles))]
        if leave:
            slots[-1] = 2
        for t, (i, c, k, w) in enumerate(tiles):
            qk(i, g, c, k, slots[t])
            if t > 0:
                j, _, k0, w0 = tiles[t - 1]
                sm_pv(j, v, w0, k0, slots[t - 1], final=final)
                if final is not None and t == hb:
                    give(range(hb - 1))
                if final is not None and t == hb + 1:
                    give([hb - 1])
            elif before is not None:
                sm_pv(*before)
        i, _, k, w = tiles[-1]
        return (i, v, w, k, slots[-1])

    @pl.when(n_steps > 0)
    def _():
        take(0)
        make_vt_half(0, 0, 0, 0)
        sm_pv(*stage(0, 0, 2, 0, 0, None, False))

    upper = [(hb * core + i, own0 + e, 0, gk, None, own_v + e, False) for e in range(2) for i in range(hb)]
    i, g, _, _, _, v, _ = upper[-1]
    upper[-1:] = [(i, g, c, 2 * ch, None, v, False) for c in (0, 2)]
    run(upper, last=False)

    def before(s):
        first = s == 1
        return (jnp.where(first, hb * core + hb - 1, CP - 1), jnp.where(first, own_v + 1, 1 - lax.rem(s, 2)), 2, 2 * ch, 2)

    def step(s, carry):
        hand_over(s - 1).wait_recv()
        take(s)
        v = lax.rem(s, 2)
        make_vt(s, v)
        stage(s, 0, 4, v, 0, before(s), True)
        return carry

    def half_steps(s, carry):
        hand_over(s - 1).wait_recv()
        v = lax.rem(s, 2)
        make_vt_half(s, 2, v, 0)
        left = stage(s, 2, 4, v, 0, before(s), False)
        take(s)
        make_vt_half(s, 0, v, 2)
        stage(s, 0, 2, v, 2, left, True)
        return carry

    n_merged = jnp.maximum(n_steps - HALVES, 1)
    lax.fori_loop(1, n_merged, step, 0)
    lax.fori_loop(n_merged, n_steps, half_steps, 0)

    def o_give(i):
        return pltpu.make_async_remote_copy(
            src_ref=out.at[CP + i], dst_ref=out.at[block_row(core, i)], send_sem=osend_sem, recv_sem=orecv_sem,
            device_id=sib_dev, device_id_type=MESH)

    def o_all():
        return pltpu.make_async_remote_copy(
            src_ref=out.at[CP:CP + hb], dst_ref=out.at[CP:CP + hb], send_sem=osend_sem, recv_sem=orecv_sem,
            device_id=sib_dev, device_id_type=MESH)

    def give(blocks):
        for i in blocks:
            o_give(i).start()

    def store_rows(i, o, l):
        inv = 1.0 / jnp.sum(l, axis=0, keepdims=True)
        out[jnp.where(i < hb, CP + i, block_row(core, i))] = (o * inv).astype(jnp.bfloat16).T.reshape(ch, rows // ch, d)

    @pl.when(n_steps > 0)
    def _():
        s = n_steps - 1
        v = 1 - lax.rem(s, 2)
        hand_over(s).wait_recv()
        make_vt_half(s + 1, 2, v, 0)
        sm_pv(*stage(s + 1, 2, 4, v, 0, before(s + 1), False, final=store_rows), final=store_rows)

    @pl.when(n_steps == 0)
    def _():
        sm_pv(hb * core + hb - 1, own_v + 1, 2, 2 * ch, 2)

        def store_block(i, carry):
            store_rows(i, acc[i], l_s[i])
            return carry
        lax.fori_loop(0, CP, store_block, 0)
        give(range(hb))

    def rest(s, carry):
        transit(s)
        return carry

    lax.fori_loop(n_steps, jnp.maximum(n_steps, n_transit), rest, 0)

    def drain(count, sem):
        def rows_of_four(i, carry):
            pltpu.make_async_remote_copy(
                src_ref=kv.at[0], dst_ref=kv.at[0], send_sem=sem, recv_sem=piece_sem, device_id=sib_dev,
                device_id_type=MESH).wait_send()
            return carry

        def single(i, carry):
            send((0, 0), (0, 0), sem, sib_dev).wait_send()
            return carry
        lax.fori_loop(0, count // 4, rows_of_four, 0)
        lax.fori_loop(0, count % 4, single, 0)

    own_up = jnp.minimum(n_up_above, CP)
    own_dn = jnp.clip(dn_top - first_dn, 0, CP)
    drain(own_up + jnp.clip(n_up_above - CP, 0, n_up) + own_dn + n_dn_below + n_transit, fwd_sem)
    drain(CP + 2 * n_steps, sib_sem)
    q_all().wait_send()
    o_all().wait_send()
    o_all().wait_recv()


def store_kernel(o_ref, out_hbm, sem):
    copy = pltpu.make_async_copy(o_ref.at[0:out_hbm.shape[0]], out_hbm, sem)
    copy.start()
    copy.wait()


def solution(mesh):
    n = mesh.shape["ctx"] // 2
    seq_spec = P("data", "ctx", None, None)

    def local_attention(queries, key_rows, value_rows):
        n_batch, chunk_len, n_heads, head_dim = queries.shape
        ch = chunk_len // CP
        rows = ch * n_heads
        n_pos = CP * (n - 1) // 2
        bf16, f32 = jnp.bfloat16, jnp.float32
        hbm = pl.BlockSpec(memory_space=pltpu.HBM)
        dma = pltpu.SemaphoreType.DMA
        out = pl.pallas_call(
            functools.partial(kernel, n, math.log2(math.e) / math.sqrt(head_dim)),
            out_shape=pltpu.VMEM((CP + CP // 2, ch, n_heads, head_dim), bf16),
            in_specs=[hbm, hbm, hbm],
            out_specs=pl.BlockSpec(memory_space=pltpu.VMEM),
            scratch_shapes=[
                pltpu.VMEM((n_pos + 5, 4, 2, ch, head_dim), bf16),
                pltpu.VMEM((CP, ch, n_heads, head_dim), bf16),
                pltpu.VMEM((CP, rows, head_dim), bf16),
                pltpu.VMEM((CP, head_dim, rows), f32),
                pltpu.VMEM((CP, 8, rows), f32),
                pltpu.VMEM((CP, 8, rows), f32),
                pltpu.VMEM((2, 4 * ch, rows), f32),
                pltpu.VMEM((2 * ch, rows), f32),
                pltpu.VMEM((3, 8, rows), f32),
                pltpu.VMEM((6, head_dim, 4 * ch), bf16),
                dma((CP,)), dma((CP // 2,)), dma((n_pos + 1, 2)), dma, dma, dma, dma, dma, dma, dma,
            ],
            compiler_params=pltpu.CompilerParams(
                collective_id=0, has_side_effects=True, vmem_limit_bytes=58 * 1024 * 1024),
            name="attention",
        )(queries.reshape(CP, ch, n_heads, head_dim), key_rows.reshape(CP, ch, head_dim),
          value_rows.reshape(CP, ch, head_dim))
        out = pl.pallas_call(
            store_kernel,
            out_shape=jax.ShapeDtypeStruct((CP, ch, n_heads, head_dim), bf16),
            in_specs=[pl.BlockSpec(memory_space=pltpu.VMEM)],
            out_specs=hbm,
            scratch_shapes=[dma],
            name="store",
        )(pltpu.with_memory_space_constraint(out, pltpu.VMEM))
        return out.reshape(queries.shape)

    return jax.shard_map(local_attention, mesh=mesh, in_specs=(seq_spec, seq_spec, seq_spec),
                         out_specs=seq_spec, check_vma=False)
```

```python
import functools
import math

import jax
import jax.numpy as jnp
from jax import lax
from jax.experimental import pallas as pl
from jax.experimental.pallas import tpu as pltpu
from jax.sharding import PartitionSpec as P

MESH = pl.DeviceIdType.MESH
CP = 8
EXTRA = 2
HALVES = 22
NT = (((1,), (1,)), ((), ()))
NN = (((1,), (0,)), ((), ()))


def kernel(n, scale2, q_hbm, k_hbm, v_hbm, out,
           kv, qraw, q_s, acc, m_s, l_s, s_s, s_left, mx_s, vt_s,
           load_sem, qload_sem, recv_sem, hand_sem, piece_sem, qrecv_sem, orecv_sem,
           fwd_sem, sib_sem, qsend_sem, osend_sem):
    me = lax.axis_index("ctx")
    chip, core = me // 2, me % 2
    sib = 1 - core
    half = n // 2
    hb = CP // 2
    n_pos = CP * (n - 1) // 2
    own0 = n_pos + 1
    ch = k_hbm.shape[1]
    d = k_hbm.shape[2]
    rows = q_s.shape[1]
    gk = 4 * ch

    def dev(c, k):
        return {"ctx": c * 2 + k}

    sib_dev = dev(chip, sib)
    above = lax.rem(chip + 1, n)
    below = lax.rem(chip + n - 1, n)
    up_dev, dn_dev = dev(above, core), dev(below, core)
    low = chip < half

    def extra(c):
        return jnp.where(c == n - 1, 0, EXTRA)

    def up_count(c):
        return jnp.where(c < half, c * CP, c * hb + extra(c))

    def up_slot(c, u):
        lo = c < half
        over = jnp.logical_and(jnp.logical_not(lo), u >= c * hb)
        row = jnp.where(lo, u // 2, jnp.where(over, u - extra(c), u))
        return row, jnp.where(lo, u % 2, over.astype(jnp.int32))

    dn_top = n_pos - extra(n - 1)
    n_up = up_count(chip)
    n_up_above = jnp.where(chip + 1 < n, up_count(chip + 1), 0)
    n_dn_below = jnp.where(chip - 1 < half, 0, (chip - 1) * hb - extra(chip - 1))
    n_steps = chip * hb
    transit0 = CP * (chip + 1)
    n_transit = jnp.where(low, jnp.maximum(dn_top - transit0, 0), 0)

    def chunk_slot(k, j):
        jj = k * CP + j
        return own0 + jj // 4, jj % 4

    def block_row(k, i):
        return 2 * (i % hb) + lax.rem(k + i, 2)

    def send(slot_from, slot_to, sem, device):
        return pltpu.make_async_remote_copy(
            src_ref=kv.at[slot_from[0], slot_from[1]], dst_ref=kv.at[slot_to[0], slot_to[1]],
            send_sem=sem, recv_sem=recv_sem.at[slot_to[0]],
            device_id=device, device_id_type=MESH)

    barrier = pltpu.get_barrier_semaphore()
    for device in (sib_dev, up_dev, dn_dev):
        pl.semaphore_signal(barrier, inc=1, device_id=device, device_id_type=MESH)

    h_chip, h_at = (n_pos - 1) // CP, CP * (n - 2) - n_pos
    is_half = core == 0

    def send_half(slot_from, slot_to, half_no, device):
        def part(slot):
            return kv.at[slot[0], slot[1], :, pl.ds(half_no * (ch // 2), ch // 2)]
        return pltpu.make_async_remote_copy(
            src_ref=part(slot_from), dst_ref=part(slot_to), send_sem=fwd_sem, recv_sem=recv_sem.at[slot_to[0]],
            device_id=device, device_id_type=MESH)

    def load_start(j):
        a, b = chunk_slot(core, j)
        pltpu.make_async_copy(k_hbm.at[j], kv.at[a, b, 0], load_sem.at[j]).start()
        pltpu.make_async_copy(v_hbm.at[j], kv.at[a, b, 1], load_sem.at[j]).start()

    def load_wait(j):
        a, b = chunk_slot(core, j)
        pltpu.make_async_copy(kv.at[a, b], kv.at[a, b], load_sem.at[j]).wait()

    for j in range(hb):
        load_start(CP - 1 - j)
        load_start(j)
    qloads = [pltpu.make_async_copy(q_hbm.at[block_row(core, hb + i)], qraw.at[hb + i], qload_sem.at[i])
              for i in range(hb)]
    for copy in qloads:
        copy.start()

    pl.semaphore_wait(barrier, 3)

    def q_give(i):
        return pltpu.make_async_remote_copy(
            src_ref=q_hbm.at[block_row(sib, i)], dst_ref=qraw.at[i], send_sem=qsend_sem, recv_sem=qrecv_sem,
            device_id=sib_dev, device_id_type=MESH)

    def q_all():
        return pltpu.make_async_remote_copy(
            src_ref=qraw.at[0:hb], dst_ref=qraw.at[0:hb], send_sem=qsend_sem, recv_sem=qrecv_sem,
            device_id=sib_dev, device_id_type=MESH)

    def piece_give():
        piece = kv.at[pl.ds(own0 + 2 * core, 2)]
        return pltpu.make_async_remote_copy(
            src_ref=piece, dst_ref=piece, send_sem=sib_sem, recv_sem=piece_sem, device_id=sib_dev, device_id_type=MESH)

    first_dn = chip * CP
    for u in range(CP):
        if u < hb:
            load_wait(CP - 1 - u)
            load_wait(u)

        split = jnp.logical_and(is_half, chip == h_chip) if u == (n_pos - 1) % CP else False

        @pl.when(jnp.logical_and(first_dn + u < dn_top, jnp.logical_not(split)))
        def _():
            send(chunk_slot(core, u), (first_dn + u, 1), fwd_sem, dn_dev).start()

        if u == (n_pos - 1) % CP:
            @pl.when(split)
            def _():
                send_half(chunk_slot(core, u), (n_pos - 1, 1), 0, dn_dev).start()

        @pl.when(u < n_up_above)
        def _():
            send(chunk_slot(core, CP - 1 - u), up_slot(chip + 1, u), fwd_sem, up_dev).start()
    for i in range(hb):
        q_give(i).start()
    piece_give().start()

    def hand_over(s):
        return pltpu.make_async_remote_copy(
            src_ref=kv.at[s, 0:2], dst_ref=kv.at[s + 1, 2:4], send_sem=sib_sem, recv_sem=hand_sem.at[lax.rem(s, 2)],
            device_id=sib_dev, device_id_type=MESH)

    def take(s):
        pltpu.make_async_remote_copy(
            src_ref=kv.at[s, 0:2], dst_ref=kv.at[s, 0:2], send_sem=sib_sem, recv_sem=recv_sem.at[s],
            device_id=sib_dev, device_id_type=MESH).wait_recv()
        hand_over(s).start()
        forward(s)

    def transit(s):
        split = jnp.logical_and(is_half, transit0 + s == n_pos - 1)

        @pl.when(jnp.logical_and(s < n_transit, jnp.logical_not(split)))
        def _():
            slot = (jnp.minimum(transit0 + s, n_pos - 1), 1)
            send(slot, slot, fwd_sem, dn_dev).wait_recv()
            send(slot, slot, fwd_sem, dn_dev).start()

        @pl.when(jnp.logical_and(s < n_transit, split))
        def _():
            slot = (n_pos - 1, 1)
            send_half(slot, slot, 0, dn_dev).wait_recv()
            send_half(slot, slot, 0, dn_dev).start()

    def forward(s):
        lo = low.astype(jnp.int32)
        p1 = s + lo * s
        p2 = p1 + lo
        up2 = up_slot(chip + 1, p2 + CP)
        to2 = (jnp.where(low, up2[0], s), jnp.where(low, up2[1], 1))
        dev2 = dev(jnp.where(low, above, below), core)

        @pl.when(p1 + CP < n_up_above)
        def _():
            send((s, 0), up_slot(chip + 1, p1 + CP), fwd_sem, up_dev).start()

        @pl.when(jnp.where(low, p2 + CP < n_up_above, s < n_dn_below))
        def _():
            send((s, 1), to2, fwd_sem, dev2).start()
        @pl.when(jnp.logical_and(is_half, jnp.logical_and(chip == n - 2, s == h_at)))
        def _():
            send_half((s, 0), (n_pos - 1, 1), 1, up_dev).start()
        transit(s)

    def score_ref(slot, nk):
        return s_left if slot == 2 else s_s.at[slot, pl.ds(0, nk)]

    def qk(i, g, c0, nk, slot, off=None):
        k = kv[g, c0:c0 + nk // ch, 0].reshape(nk, d)
        s = lax.dot_general(k, q_s[i], NT, preferred_element_type=jnp.float32)
        if off is not None:
            key = lax.broadcasted_iota(jnp.int32, (nk, rows), 0)
            tok = lax.broadcasted_iota(jnp.int32, (nk, rows), 1) // 2
            s = jnp.where(key - tok <= off, s, -jnp.inf)
        score_ref(slot, nk)[...] = s
        mx_s[slot] = jnp.max(s.reshape(nk // 8, 8, rows), axis=0)

    def sm_pv(i, v, c0, nk, slot, first=False, final=None):
        m_new = jnp.max(mx_s[slot], axis=0, keepdims=True)
        if first:
            m_new = jnp.broadcast_to(m_new, (8, rows))
        else:
            m_old = m_s[i]
            m_new = jnp.maximum(m_old, m_new)
            alpha = jnp.exp2((m_old - m_new) * scale2)
        if final is None:
            m_s[i] = m_new
        p = jnp.exp2((score_ref(slot, nk)[...].reshape(nk // 8, 8, rows) - m_new[None]) * scale2)
        l_new = jnp.sum(p, axis=0)
        pv = lax.dot_general(vt_s[v, :, c0 * ch:c0 * ch + nk], p.reshape(nk, rows).astype(jnp.bfloat16), NN,
                             preferred_element_type=jnp.float32)
        if first:
            l_s[i] = l_new
            acc[i] = pv
            return
        l_new = l_s[i] * alpha + l_new
        o = (acc[i].reshape(d // 8, 8, rows) * alpha[None]).reshape(d, rows) + pv
        if final is None:
            l_s[i] = l_new
            acc[i] = o
        else:
            final(i, o, l_new)

    def make_vt(g, v):
        vt_s[v] = kv[g, :, 1].reshape(gk, d).T

    def make_vt_half(g, c0, v, v0):
        vt_s[v, :, v0 * ch:(v0 + 2) * ch] = kv[g, c0:c0 + 2, 1].reshape(2 * ch, d).T

    own_v = 2

    def run(tiles, last=True):
        def slot(t):
            return 2 if t == len(tiles) - 1 and not last else t % 2

        def scores(t):
            i, g, c0, nk, off, v, first = tiles[t]
            qk(i, g, c0, nk, slot(t), off)

        scores(0)
        for t, (i, g, c0, nk, off, v, first) in enumerate(tiles):
            if t + 1 < len(tiles):
                scores(t + 1)
            elif not last:
                break
            sm_pv(i, v, c0, nk, slot(t), first)

    def triangle(k, i0):
        for i in range(hb):
            q_s[i0 + i] = qraw[i0 + i].reshape(rows, d)
        for e in range(2):
            make_vt(own0 + 2 * k + e, own_v + 2 * k + e)
        tiles = []
        for i in range(hb):
            for e in range(i // 2 + 1):
                g, v = own0 + 2 * k + e, own_v + 2 * k + e
                if e < i // 2:
                    tiles.append((i0 + i, g, 0, gk, None, v, e == 0))
                elif i % 2 == 0:
                    tiles.append((i0 + i, g, 0, 2 * ch, ch * core, v, e == 0))
                else:
                    tiles.append((i0 + i, g, 0, gk, ch * (3 - core), v, e == 0))
        run(tiles)

    for copy in qloads:
        copy.wait()
    triangle(core, hb)
    q_all().wait_recv()
    piece_give().wait_recv()
    triangle(sib, 0)

    def stage(g, c0, c1, v, v0, before, leave, final=None):
        nk = (c1 - c0) * ch
        tiles = [(i, c0, nk, v0) for i in range(CP)]
        if leave and c1 - c0 > 2:
            tiles[-1:] = [(CP - 1, c0, 2 * ch, v0), (CP - 1, c0 + 2, 2 * ch, v0 + 2)]
        slots = [t % 2 for t in range(len(tiles))]
        if leave:
            slots[-1] = 2
        for t, (i, c, k, w) in enumerate(tiles):
            qk(i, g, c, k, slots[t])
            if t > 0:
                j, _, k0, w0 = tiles[t - 1]
                sm_pv(j, v, w0, k0, slots[t - 1], final=final)
                if final is not None and t == hb:
                    give(range(hb - 1))
                if final is not None and t == hb + 1:
                    give([hb - 1])
            elif before is not None:
                sm_pv(*before)
        i, _, k, w = tiles[-1]
        return (i, v, w, k, slots[-1])

    @pl.when(n_steps > 0)
    def _():
        take(0)
        make_vt_half(0, 0, 0, 0)
        sm_pv(*stage(0, 0, 2, 0, 0, None, False))

    upper = [(hb * core + i, own0 + e, 0, gk, None, own_v + e, False) for e in range(2) for i in range(hb)]
    i, g, _, _, _, v, _ = upper[-1]
    upper[-1:] = [(i, g, c, 2 * ch, None, v, False) for c in (0, 2)]
    run(upper, last=False)

    def before(s):
        first = s == 1
        return (jnp.where(first, hb * core + hb - 1, CP - 1), jnp.where(first, own_v + 1, 1 - lax.rem(s, 2)), 2, 2 * ch, 2)

    def step(s, carry):
        hand_over(s - 1).wait_recv()
        take(s)
        v = lax.rem(s, 2)
        make_vt(s, v)
        stage(s, 0, 4, v, 0, before(s), True)
        return carry

    def half_steps(s, carry):
        hand_over(s - 1).wait_recv()
        v = lax.rem(s, 2)
        make_vt_half(s, 2, v, 0)
        left = stage(s, 2, 4, v, 0, before(s), False)
        take(s)
        make_vt_half(s, 0, v, 2)
        stage(s, 0, 2, v, 2, left, True)
        return carry

    n_merged = jnp.maximum(n_steps - HALVES, 1)
    lax.fori_loop(1, n_merged, step, 0)
    lax.fori_loop(n_merged, n_steps, half_steps, 0)

    def o_give(i):
        return pltpu.make_async_remote_copy(
            src_ref=out.at[CP + i], dst_ref=out.at[block_row(core, i)], send_sem=osend_sem, recv_sem=orecv_sem,
            device_id=sib_dev, device_id_type=MESH)

    def o_all():
        return pltpu.make_async_remote_copy(
            src_ref=out.at[CP:CP + hb], dst_ref=out.at[CP:CP + hb], send_sem=osend_sem, recv_sem=orecv_sem,
            device_id=sib_dev, device_id_type=MESH)

    def give(blocks):
        for i in blocks:
            o_give(i).start()

    def store_rows(i, o, l):
        inv = 1.0 / jnp.sum(l, axis=0, keepdims=True)
        out[jnp.where(i < hb, CP + i, block_row(core, i))] = (o * inv).astype(jnp.bfloat16).T.reshape(ch, rows // ch, d)

    @pl.when(n_steps > 0)
    def _():
        s = n_steps - 1
        v = 1 - lax.rem(s, 2)
        hand_over(s).wait_recv()
        make_vt_half(s + 1, 2, v, 0)
        sm_pv(*stage(s + 1, 2, 4, v, 0, before(s + 1), False, final=store_rows), final=store_rows)

    @pl.when(n_steps == 0)
    def _():
        sm_pv(hb * core + hb - 1, own_v + 1, 2, 2 * ch, 2)

        def store_block(i, carry):
            store_rows(i, acc[i], l_s[i])
            return carry
        lax.fori_loop(0, CP, store_block, 0)
        give(range(hb))

    def rest(s, carry):
        transit(s)
        return carry

    lax.fori_loop(n_steps, jnp.maximum(n_steps, n_transit), rest, 0)

    def drain(count, sem):
        def rows_of_four(i, carry):
            pltpu.make_async_remote_copy(
                src_ref=kv.at[0], dst_ref=kv.at[0], send_sem=sem, recv_sem=piece_sem, device_id=sib_dev,
                device_id_type=MESH).wait_send()
            return carry

        def single(i, carry):
            send((0, 0), (0, 0), sem, sib_dev).wait_send()
            return carry
        lax.fori_loop(0, count // 4, rows_of_four, 0)
        lax.fori_loop(0, count % 4, single, 0)

    own_up = jnp.minimum(n_up_above, CP)
    own_dn = jnp.clip(dn_top - first_dn, 0, CP)
    n_split = jnp.where(jnp.logical_and(is_half, chip <= h_chip), 1, 0)
    drain(own_up + jnp.clip(n_up_above - CP, 0, n_up) + own_dn + n_dn_below + n_transit - n_split, fwd_sem)

    @pl.when(jnp.logical_and(is_half, jnp.logical_or(chip <= h_chip, chip == n - 2)))
    def _():
        send_half((0, 0), (0, 0), 0, sib_dev).wait_send()
    drain(CP + 2 * n_steps, sib_sem)
    q_all().wait_send()
    o_all().wait_send()
    o_all().wait_recv()


def store_kernel(o_ref, out_hbm, sem):
    copy = pltpu.make_async_copy(o_ref.at[0:out_hbm.shape[0]], out_hbm, sem)
    copy.start()
    copy.wait()


def solution(mesh):
    n = mesh.shape["ctx"] // 2
    seq_spec = P("data", "ctx", None, None)

    def local_attention(queries, key_rows, value_rows):
        n_batch, chunk_len, n_heads, head_dim = queries.shape
        ch = chunk_len // CP
        rows = ch * n_heads
        n_pos = CP * (n - 1) // 2
        bf16, f32 = jnp.bfloat16, jnp.float32
        hbm = pl.BlockSpec(memory_space=pltpu.HBM)
        dma = pltpu.SemaphoreType.DMA
        out = pl.pallas_call(
            functools.partial(kernel, n, math.log2(math.e) / math.sqrt(head_dim)),
            out_shape=pltpu.VMEM((CP + CP // 2, ch, n_heads, head_dim), bf16),
            in_specs=[hbm, hbm, hbm],
            out_specs=pl.BlockSpec(memory_space=pltpu.VMEM),
            scratch_shapes=[
                pltpu.VMEM((n_pos + 5, 4, 2, ch, head_dim), bf16),
                pltpu.VMEM((CP, ch, n_heads, head_dim), bf16),
                pltpu.VMEM((CP, rows, head_dim), bf16),
                pltpu.VMEM((CP, head_dim, rows), f32),
                pltpu.VMEM((CP, 8, rows), f32),
                pltpu.VMEM((CP, 8, rows), f32),
                pltpu.VMEM((2, 4 * ch, rows), f32),
                pltpu.VMEM((2 * ch, rows), f32),
                pltpu.VMEM((3, 8, rows), f32),
                pltpu.VMEM((6, head_dim, 4 * ch), bf16),
                dma((CP,)), dma((CP // 2,)), dma((n_pos,)), dma((2,)), dma, dma, dma, dma, dma, dma, dma,
            ],
            compiler_params=pltpu.CompilerParams(
                collective_id=0, has_side_effects=True, vmem_limit_bytes=58 * 1024 * 1024),
            name="attention",
        )(queries.reshape(CP, ch, n_heads, head_dim), key_rows.reshape(CP, ch, head_dim),
          value_rows.reshape(CP, ch, head_dim))
        out = pl.pallas_call(
            store_kernel,
            out_shape=jax.ShapeDtypeStruct((CP, ch, n_heads, head_dim), bf16),
            in_specs=[pl.BlockSpec(memory_space=pltpu.VMEM)],
            out_specs=hbm,
            scratch_shapes=[dma],
            name="store",
        )(pltpu.with_memory_space_constraint(out, pltpu.VMEM))
        return out.reshape(queries.shape)

    return jax.shard_map(local_attention, mesh=mesh, in_specs=(seq_spec, seq_spec, seq_spec),
                         out_specs=seq_spec, check_vma=False)
```
